128 devices in a mesh: dp: 8 (over x_lo, z), seq: 16 (over y, x_hi, core).
Axes of the slice: x: 4 (x_hi: 2, x_lo: 2; x = x_hi * 2 + x_lo), y: 4, z: 4, core: 2. Of those that a mesh axis runs over, the one named last changes fastest.
Arguments:
- query_rows: bfloat16 [8, 6144, 1024], P('dp', 'seq'), may hold values from -48 to 48
- key_rows: bfloat16 [8, 6144, 1024], P('dp', 'seq'), may hold values from -8 to 8
- value_rows: bfloat16 [8, 6144, 1024], P('dp', 'seq'), may hold values from -6 to 6
- scale_end: int32 [6144], P('seq'), may hold values from 1 to 6144, as said below
- out_weight: bfloat16 [1024, 2048], replicated, may hold values from -0.8984375 to 0.8984375
- grad_out: bfloat16 [8, 6144, 2048], P('dp', 'seq'), may hold values from -0.75 to 0.75
Outputs:
- mixed_out: bfloat16 [8, 6144, 2048], P('dp', 'seq')
- out_grad: float32 [1024, 2048], P(('dp', 'seq'))
The draws below stay inside these ranges and needn't reach their ends.
Inputs may be any that keep to these rules, and one draw needn't show every extreme that they name: scale_end is constant over each of 4 scales of consecutive tokens, equals the index one past the scale's last token (so scale_end[t] > t), never falls, and is 6144 on the last scale; the same for every image.
All inputs are finite; a program needn't handle non-finite values.
Results may differ from the reference program's by a relative error of at most 0.014.
Values may be sent and summed in bfloat16 or wider, within the bound.
A program may use at most 256 MiB of HBM per device.

```python
import jax
import jax.numpy as jnp
from jax import lax

D = 2048
HEADS = 8
HEAD = 128
SCALES = 4
HD = 1024
TOKENS = 6144
IMAGES = 8


def query_key_pair(key):
    base = jax.random.fold_in(key, 7101)
    query_key, key_key = jax.random.split(base, 2)
    shape = (IMAGES, TOKENS, HD)
    key_values = jnp.clip(1.2 * jax.random.normal(key_key, shape, jnp.float32), -7.0, 7.0)
    query_values = jnp.clip(jax.random.normal(query_key, shape, jnp.float32), -6.0, 6.0)
    return (query_values, key_values)


def draw_query_rows(key, part):
    query_values, key_values = query_key_pair(key)
    return query_values.astype(jnp.bfloat16)


def draw_key_rows(key, part):
    query_values, key_values = query_key_pair(key)
    return key_values.astype(jnp.bfloat16)


def draw_scale_end(key, part):
    local_key = jax.random.fold_in(key, 7203)
    picks = jax.random.permutation(local_key, TOKENS - 1)[:SCALES - 1].astype(jnp.int32) + 1
    cuts = jnp.sort(picks)
    ends = jnp.concatenate([cuts, jnp.full((1,), TOKENS, jnp.int32)]).astype(jnp.int32)
    positions = jnp.arange(TOKENS, dtype=jnp.int32)
    chosen = jnp.where(ends[None, :] > positions[:, None], ends[None, :], TOKENS)
    return jnp.min(chosen, axis=1).astype(jnp.int32)


def level_of(own_key, extent, cuts, smallest, high):
    def one(axis_at, shards_of):
        draws = jax.random.uniform(jax.random.fold_in(jax.random.fold_in(own_key, 6), axis_at), (shards_of,), jnp.float32, smallest / len(cuts), high / len(cuts))
        return jnp.repeat(jnp.exp(draws), extent[axis_at] // shards_of).reshape((-1,) + (1,) * (len(extent) - axis_at - 1))

    factor_of = one(*cuts[0])
    for cut in cuts[1:]:
        factor_of = factor_of * one(*cut)
    return factor_of


def normal_values(stream_key, shape, spread, limit, pieces=(), kind=jnp.bfloat16):
    drawn = spread * jax.random.normal(stream_key, shape, jnp.float32)
    if pieces:
        drawn = drawn * level_of(stream_key, shape, pieces, -0.22, 0.18)
    return jnp.clip(drawn, -limit, limit).astype(kind)


def setup_inputs(seed: int = 0) -> dict:
    key_list = jax.random.split(jax.random.key(seed), 7)
    return {
        "query_rows": draw_query_rows(jax.random.fold_in(key_list[6], 71), 0),
        "key_rows": draw_key_rows(jax.random.fold_in(key_list[6], 71), 0),
        "value_rows": normal_values(key_list[2], (IMAGES, TOKENS, HD), 1.0, 6.0, ((0, 8), (1, 16))),
        "scale_end": draw_scale_end(jax.random.fold_in(key_list[6], 71), 0),
        "out_weight": jnp.clip(jax.random.uniform(key_list[4], (HD, D), jnp.float32, -0.8984375, 0.8984375), -0.8984375, 0.8984375).astype(jnp.bfloat16),
        "grad_out": normal_values(key_list[5], (IMAGES, TOKENS, D), (12.0 / (TOKENS * IMAGES) ** 0.5), 0.75, ((0, 8), (1, 16))),
    }


floor_score = -1.0e30


def reference(query_rows, key_rows, value_rows, scale_end, out_weight, grad_out):
    positions = jnp.arange(TOKENS, dtype=jnp.int32)
    visible = positions[None, :] < scale_end[:, None]

    def one_head(triple):
        query_head, key_head, value_head = triple
        scores = jnp.dot(query_head, key_head.T, preferred_element_type=jnp.float32) * (HEAD ** -0.5)
        masked = jnp.where(visible, scores, floor_score)
        row_max = jnp.max(masked, axis=1, keepdims=True)
        weights = jnp.where(visible, jnp.exp(masked - row_max), 0.0)
        row_sum = jnp.sum(weights, axis=1, keepdims=True)
        mixed_values = jnp.dot(weights.astype(jnp.bfloat16), value_head, preferred_element_type=jnp.float32)
        return (mixed_values / row_sum).astype(jnp.bfloat16)

    def split_heads(matrix):
        return matrix.reshape(TOKENS, HEADS, HEAD).transpose(1, 0, 2)

    def one_image(triple):
        query_img, key_img, value_img = triple
        outputs = lax.map(one_head, (split_heads(query_img), split_heads(key_img), split_heads(value_img)))
        return outputs.transpose(1, 0, 2).reshape(TOKENS, HD)

    attended = lax.map(one_image, (query_rows, key_rows, value_rows))
    flat_attended = attended.reshape(IMAGES * TOKENS, HD)
    mixed_out = jnp.dot(flat_attended, out_weight, preferred_element_type=jnp.float32).astype(jnp.bfloat16)
    mixed_out = mixed_out.reshape(IMAGES, TOKENS, D)
    out_grad = jnp.dot(flat_attended.T, grad_out.reshape(IMAGES * TOKENS, D), preferred_element_type=jnp.float32)
    return (mixed_out, out_grad)
```

```python
import functools
import math

import jax
import jax.numpy as jnp
from jax import lax
from jax.experimental import pallas as pl
from jax.experimental.pallas import tpu as pltpu
from jax.sharding import Mesh
from jax.sharding import PartitionSpec as P

HEAD = 128
DP = ("dp_0", "dp_1")
DP_SEQ = ("dp_0", "dp_1", "seq")
MESH = pl.DeviceIdType.MESH
LOG2_SCALE = HEAD ** (-0.5) * math.log2(math.e)
LOW = -1e30
HIDE = -(2.0**100)
CHIPS = 8
WIDE = 256
GROUP = 4
ONES = 16


def in_blocks(array, dim, count):
    before, after = (array.shape[:dim], array.shape[dim + 1 :])
    return jnp.moveaxis(array.reshape(*before, count, -1, *after), dim, 0)


def own_block(tiles, axes, order):
    shape = [lax.axis_size(a) for a in axes]
    tiles = tiles.reshape(*shape, *tiles.shape[1:])
    tiles = tiles.transpose(*order, *range(len(axes), tiles.ndim))
    tiles = tiles.reshape(-1, *tiles.shape[len(axes) :])
    for k in order:
        tiles = lax.psum_scatter(tiles, axes[k], scatter_dimension=0, tiled=True)
    return tiles[0]


def scatter_axes(array, axes, order, dim):
    count = lax.axis_size(axes)
    return own_block(in_blocks(array, dim, count), axes, order)


def sent_and_summed(array, axis, dim):
    count = lax.axis_size(axis)
    tiles = lax.all_to_all(in_blocks(array, dim, count), axis, 0, 0, tiled=True)
    return jnp.sum(tiles.astype(jnp.float32), axis=0)


def attend_kernel(
    rows,
    q_ref, k_ref, v_ref, end_ref, out_ref,
    qq, kk, vals, vt, ends, acc, top, sbuf, sbuf_top, obuf,
    local_sem, q_send, q_recv, kv_send, kv_recv, f_send, f_recv, e_send, e_recv, o_send, o_recv,
):
    seq = lax.axis_index("seq")
    chip = seq // 2
    core = seq % 2
    row_y = chip // 2
    col_x = chip % 2
    pair = 2 * rows
    tokens = CHIPS * pair
    mine = CHIPS * rows
    steps = mine // (WIDE * GROUP)

    def chip_at(b, sign):
        part = b // 2
        dy = part + part // 2 - 2 * (part // 3)
        return ((row_y + sign * dy + 4) % 4) * 2 + (col_x + b % 2) % 2

    barrier = pltpu.get_barrier_semaphore()
    for i in range(1, 2 * CHIPS):
        pl.semaphore_signal(
            barrier, inc=1, device_id={"seq": (seq + i) % (2 * CHIPS)}, device_id_type=MESH
        )
    pl.semaphore_wait(barrier, 2 * CHIPS - 1)

    def cols(head):
        return pl.ds(pl.multiple_of(head * HEAD, HEAD), HEAD)

    def token_rows(c, j):
        return pl.ds(pl.multiple_of((c * 2 + j) * rows, rows), rows)

    def query_rows(c):
        return pl.ds(pl.multiple_of(c * rows, rows), rows)

    def remote(src, dst, send, recv, c, j):
        return pltpu.make_async_remote_copy(
            src_ref=src, dst_ref=dst, send_sem=send, recv_sem=recv,
            device_id={"seq": c * 2 + j}, device_id_type=MESH,
        )

    def end_copy(i, to):
        return pltpu.make_async_remote_copy(
            src_ref=end_ref, dst_ref=ends.at[seq], send_sem=e_send.at[i], recv_sem=e_recv.at[i],
            device_id={"seq": to}, device_id_type=MESH,
        )

    def q_copy(b):
        to = chip_at(b, 1)
        return remote(
            q_ref.at[:, cols(to)], qq.at[query_rows(chip), 0:HEAD], q_send.at[b], q_recv.at[b], to, core
        )

    def k_copy(b):
        to = chip_at(b, 1)
        return remote(
            k_ref.at[:, cols(to)], kk.at[token_rows(chip, core), 0:HEAD],
            kv_send.at[0, b], kv_recv.at[0, b], to, core,
        )

    def v_copy(b):
        to = chip_at(b, 1)
        return remote(
            v_ref.at[:, cols(to)], vals.at[token_rows(chip, core), :],
            kv_send.at[1, b], kv_recv.at[1, b], to, core,
        )

    def forward_k(b):
        at = token_rows(chip_at(b, -1), core)
        return remote(
            kk.at[at, 0:HEAD], kk.at[at, 0:HEAD], f_send.at[0, b], f_recv.at[0, b], chip, 1 - core
        )

    def forward_v(b):
        at = token_rows(chip_at(b, -1), core)
        return remote(
            vals.at[at, :], vals.at[at, :], f_send.at[1, b], f_recv.at[1, b], chip, 1 - core
        )

    own = [
        pltpu.make_async_copy(
            k_ref.at[:, cols(chip)], kk.at[token_rows(chip, core), 0:HEAD], local_sem.at[0]
        ),
        pltpu.make_async_copy(
            v_ref.at[:, cols(chip)], vals.at[token_rows(chip, core), :], local_sem.at[1]
        ),
        pltpu.make_async_copy(
            q_ref.at[:, cols(chip)], qq.at[query_rows(chip), 0:HEAD], local_sem.at[2]
        ),
        pltpu.make_async_copy(end_ref, ends.at[seq], local_sem.at[3]),
    ]
    for i in range(1, 2 * CHIPS):
        end_copy(i, (seq + i) % (2 * CHIPS)).start()
    for copy in own:
        copy.start()
    for b in range(1, CHIPS):
        q_copy(b).start()
    for b in range(1, CHIPS):
        k_copy(b).start()
        v_copy(b).start()
    own[0].wait()
    forward_k(0).start()
    own[1].wait()
    forward_v(0).start()

    vt[HEAD:, :] = jnp.ones((ONES, tokens), jnp.bfloat16)
    acc[...] = jnp.zeros_like(acc)
    top[...] = jnp.full_like(top, LOW)
    own[2].wait()
    own[3].wait()
    for i in range(1, 2 * CHIPS):
        end_copy(i, (seq + i) % (2 * CHIPS)).wait()

    every = ends[...].reshape(2 * CHIPS * 8, rows).astype(jnp.float32)

    def least(x):
        return jnp.min(jnp.min(x, axis=0, keepdims=True), axis=1, keepdims=True)

    whole = jnp.float32(tokens)
    first = least(every)
    second = least(jnp.where(every > first, every, whole))
    third = least(jnp.where(every > second, every, whole))
    lane = lax.broadcasted_iota(jnp.int32, (8, HEAD), 1)
    stop = jnp.where(lane == 0, first, jnp.where(lane == 1, second, jnp.where(lane == 2, third, whole)))
    start = jnp.where(
        lane == 0, jnp.float32(0), jnp.where(lane == 1, first, jnp.where(lane == 2, second, third))
    )
    start = jnp.where(lane < 4, start, 2.0 * whole)[0:1, :]
    stop = stop[0:1, :]

    def hide_keys(i, unused):
        base = pl.multiple_of(i * pair, pair)
        at = (base + lax.broadcasted_iota(jnp.int32, (pair, HEAD), 0)).astype(jnp.float32)
        kk[pl.ds(base, pair), HEAD:] = jnp.where(at >= stop, HIDE, 0.0).astype(jnp.bfloat16)
        return unused

    lax.fori_loop(0, CHIPS, hide_keys, 0)

    def mark_queries(i, unused):
        base = (i * 2 + core) * rows
        at = (base + lax.broadcasted_iota(jnp.int32, (rows, HEAD), 0)).astype(jnp.float32)
        inside = jnp.where(at >= start, 1.0, 0.0) * jnp.where(at < stop, 1.0, 0.0)
        qq[query_rows(i), HEAD:] = inside.astype(jnp.bfloat16)
        return unused

    lax.fori_loop(0, CHIPS, mark_queries, 0)
    for b in range(1, CHIPS):
        q_copy(b).wait_recv()

    def block_rows(b):
        return pl.ds(pl.multiple_of(chip_at(b, -1) * pair, pair), pair)

    def pass_on(b):
        k_copy(b).wait_recv()
        forward_k(b).start()
        v_copy(b).wait_recv()
        forward_v(b).start()

    def receive(b):
        forward_k(b).wait_recv()
        forward_v(b).wait_recv()
        at = block_rows(b)
        vt[0:HEAD, at] = vals[at, :].T

    def fill(b, step, u):
        queries = pl.ds(pl.multiple_of(step * WIDE, WIDE), WIDE)
        scores = lax.dot_general(
            kk[block_rows(b), :], qq[queries, :], (((1,), (1,)), ((), ())),
            preferred_element_type=jnp.float32,
        )
        sbuf_top[u, 0:1, :] = jnp.max(scores, axis=0, keepdims=True)
        sbuf[u] = scores

    def use(b, step, u):
        queries = pl.ds(pl.multiple_of(step * WIDE, WIDE), WIDE)
        old = top[0:1, queries]
        new = jnp.maximum(old, sbuf_top[u, 0:1, :])
        top[0:1, queries] = new
        weights = jnp.exp2(sbuf[u] * LOG2_SCALE - new * LOG2_SCALE).astype(jnp.bfloat16)
        factor = jnp.exp2((old - new) * LOG2_SCALE)
        product = jnp.dot(vt[:, block_rows(b)], weights, preferred_element_type=jnp.float32)
        acc[:, queries] = acc[:, queries] * factor + product

    receive(0)
    for u in range(GROUP):
        fill(0, u, u)

    def body(t, unused):
        b = t // steps
        i = t % steps

        @pl.when((i == steps - 2) & (b < CHIPS - 1))
        def _():
            pass_on(b + 1)

        @pl.when((i == steps - 1) & (b < CHIPS - 1))
        def _():
            receive(b + 1)

        later = jnp.minimum(t + 1, CHIPS * steps - 1)
        for u in range(GROUP):
            use(b, i * GROUP + u, u)
            fill(later // steps, (later % steps) * GROUP + u, u)
        return unused

    lax.fori_loop(0, CHIPS * steps, body, 0)

    def out_copy(b):
        to = chip_at(b, 1)
        return remote(
            obuf.at[query_rows(to), :], out_ref.at[:, cols(chip)], o_send.at[b], o_recv.at[b], to, core
        )

    own_out = pltpu.make_async_copy(
        obuf.at[query_rows(chip), :], out_ref.at[:, cols(chip)], local_sem.at[4]
    )
    for b in (*range(1, CHIPS), 0):
        at = query_rows(chip_at(b, 1))
        whole_sum = acc[HEAD : HEAD + 1, at]
        obuf[at, :] = (acc[0:HEAD, at] / whole_sum).T.astype(jnp.bfloat16)
        if b:
            out_copy(b).start()
        else:
            own_out.start()

    for b in range(1, CHIPS):
        q_copy(b).wait_send()
        k_copy(b).wait_send()
        v_copy(b).wait_send()
    for b in range(CHIPS):
        forward_k(b).wait_send()
        forward_v(b).wait_send()
    for b in range(1, CHIPS):
        out_copy(b).wait()
    own_out.wait()


def attend(q, k, v, ends):
    rows, width = q.shape
    pair = 2 * rows
    tokens = CHIPS * pair
    mine = CHIPS * rows
    any_space = pl.BlockSpec(memory_space=pl.ANY)
    dma = pltpu.SemaphoreType.DMA
    return pl.pallas_call(
        functools.partial(attend_kernel, rows),
        out_shape=jax.ShapeDtypeStruct((rows, width), jnp.bfloat16),
        in_specs=[any_space] * 4,
        out_specs=any_space,
        scratch_shapes=[
            pltpu.VMEM((mine, 2 * HEAD), jnp.bfloat16),
            pltpu.VMEM((tokens, 2 * HEAD), jnp.bfloat16),
            pltpu.VMEM((tokens, HEAD), jnp.bfloat16),
            pltpu.VMEM((HEAD + ONES, tokens), jnp.bfloat16),
            pltpu.VMEM((2 * CHIPS, 8, rows), jnp.int32),
            pltpu.VMEM((HEAD + ONES, mine), jnp.float32),
            pltpu.VMEM((8, mine), jnp.float32),
            pltpu.VMEM((GROUP, pair, WIDE), jnp.float32),
            pltpu.VMEM((GROUP, 8, WIDE), jnp.float32),
            pltpu.VMEM((mine, HEAD), jnp.bfloat16),
            dma((5,)),
            dma((CHIPS,)), dma((CHIPS,)),
            dma((2, CHIPS)), dma((2, CHIPS)),
            dma((2, CHIPS)), dma((2, CHIPS)),
            dma((2 * CHIPS,)), dma((2 * CHIPS,)),
            dma((CHIPS,)), dma((CHIPS,)),
        ],
        compiler_params=pltpu.CompilerParams(
            collective_id=0, has_side_effects=True, vmem_limit_bytes=60 << 20
        ),
    )(q, k, v, ends)


def body(query_rows, key_rows, value_rows, scale_end, out_weight, grad_out):
    rows = query_rows.shape[1]
    ends = jnp.broadcast_to(scale_end[None, :], (8, rows))
    attended = attend(query_rows[0], key_rows[0], value_rows[0], ends)
    mixed_out = jnp.dot(attended, out_weight, preferred_element_type=jnp.float32).astype(
        jnp.bfloat16
    )[None]
    local_grad = grad_out[0]
    shares = scatter_axes(
        lax.dot_general(
            attended, local_grad, (((0,), (0,)), ((), ())), preferred_element_type=jnp.float32
        ).astype(jnp.bfloat16),
        DP,
        (1, 0),
        0,
    ).astype(jnp.float32)
    grad_shard = sent_and_summed(shares.astype(jnp.bfloat16), "seq", 0)
    return (mixed_out, grad_shard)


def solution(mesh):
    torus = Mesh(mesh.devices.reshape(2, 4, mesh.shape["seq"]), ("dp_0", "dp_1", "seq"))
    in_specs = (
        P(DP, "seq", None),
        P(DP, "seq", None),
        P(DP, "seq", None),
        P("seq"),
        P(),
        P(DP, "seq", None),
    )
    out_specs = (P(DP, "seq", None), P(DP_SEQ, None))
    return jax.shard_map(body, mesh=torus, in_specs=in_specs, out_specs=out_specs, check_vma=False)
```

```python
import functools
import math

import jax
import jax.numpy as jnp
from jax import lax
from jax.experimental import pallas as pl
from jax.experimental.pallas import tpu as pltpu
from jax.sharding import Mesh
from jax.sharding import PartitionSpec as P

HEAD = 128
DP = ("dp_0", "dp_1")
PARTS = (384, 384, 256)
ORDERS = ("zyx", "yxz", "xzy")
DP_SEQ = ("dp_0", "dp_1", "seq")
MESH = pl.DeviceIdType.MESH
LOG2_SCALE = HEAD ** (-0.5) * math.log2(math.e)
LOW = -1e30
HIDE = -(2.0**100)
CHIPS = 8
WIDE = 256
GROUP = 4
ONES = 16


def attend_kernel(
    rows,
    q_ref, k_ref, v_ref, end_ref, w_ref, g_ref, mixed_ref, grad_ref,
    qq, kk, vals, vt, ends, acc, top, sbuf, sbuf_top, obuf,
    local_sem, q_send, q_recv, kv_send, kv_recv, f_send, f_recv, e_send, e_recv, o_send, o_recv,
    att, w_buf, g_own, g_sib, mixed, part_own, part_sib, part_in, tiles, landed, totals, grad,
    c_send, c_recv, r_send, r_recv, s_sem,
):
    seq = lax.axis_index("seq")
    x_lo = lax.axis_index("dp_0")
    z = lax.axis_index("dp_1")
    half = g_own.shape[1]
    chip = seq // 2
    core = seq % 2
    row_y = chip // 2
    col_x = chip % 2
    pair = 2 * rows
    tokens = CHIPS * pair
    mine = CHIPS * rows
    steps = mine // (WIDE * GROUP)

    def chip_at(b, sign):
        part = b // 2
        dy = part + part // 2 - 2 * (part // 3)
        return ((row_y + sign * dy + 4) % 4) * 2 + (col_x + b % 2) % 2

    barrier = pltpu.get_barrier_semaphore()
    for i in range(1, 2 * CHIPS):
        pl.semaphore_signal(
            barrier, inc=1, device_id={"seq": (seq + i) % (2 * CHIPS)}, device_id_type=MESH
        )
    x = col_x * 2 + x_lo

    def peer(axis, d):
        if axis == "z":
            return {"dp_1": (z + d) % 4}
        if axis == "y":
            return {"seq": ((row_y + d) % 4) * 4 + col_x * 2 + core}
        to = (x + d) % 4
        return {"dp_0": to % 2, "seq": row_y * 4 + (to // 2) * 2 + core}

    for axis, d in (("x", 1), ("x", 3), ("z", 1), ("z", 2), ("z", 3)):
        pl.semaphore_signal(barrier, inc=1, device_id=peer(axis, d), device_id_type=MESH)
    pl.semaphore_wait(barrier, 2 * CHIPS + 4)

    def cols(head):
        return pl.ds(pl.multiple_of(head * HEAD, HEAD), HEAD)

    def token_rows(c, j):
        return pl.ds(pl.multiple_of((c * 2 + j) * rows, rows), rows)

    def query_rows(c):
        return pl.ds(pl.multiple_of(c * rows, rows), rows)

    def remote(src, dst, send, recv, c, j):
        return pltpu.make_async_remote_copy(
            src_ref=src, dst_ref=dst, send_sem=send, recv_sem=recv,
            device_id={"seq": c * 2 + j}, device_id_type=MESH,
        )

    def end_copy(i, to):
        return pltpu.make_async_remote_copy(
            src_ref=end_ref, dst_ref=ends.at[seq], send_sem=e_send.at[i], recv_sem=e_recv.at[i],
            device_id={"seq": to}, device_id_type=MESH,
        )

    def q_copy(b):
        to = chip_at(b, 1)
        return remote(
            q_ref.at[:, cols(to)], qq.at[query_rows(chip), 0:HEAD], q_send.at[b], q_recv.at[b], to, core
        )

    def k_copy(b):
        to = chip_at(b, 1)
        return remote(
            k_ref.at[:, cols(to)], kk.at[token_rows(chip, core), 0:HEAD],
            kv_send.at[0, b], kv_recv.at[0, b], to, core,
        )

    def v_copy(b):
        to = chip_at(b, 1)
        return remote(
            v_ref.at[:, cols(to)], vals.at[token_rows(chip, core), :],
            kv_send.at[1, b], kv_recv.at[1, b], to, core,
        )

    def forward_k(b):
        at = token_rows(chip_at(b, -1), core)
        return remote(
            kk.at[at, 0:HEAD], kk.at[at, 0:HEAD], f_send.at[0, b], f_recv.at[0, b], chip, 1 - core
        )

    def forward_v(b):
        at = token_rows(chip_at(b, -1), core)
        return remote(
            vals.at[at, :], vals.at[at, :], f_send.at[1, b], f_recv.at[1, b], chip, 1 - core
        )

    own = [
        pltpu.make_async_copy(
            k_ref.at[:, cols(chip)], kk.at[token_rows(chip, core), 0:HEAD], local_sem.at[0]
        ),
        pltpu.make_async_copy(
            v_ref.at[:, cols(chip)], vals.at[token_rows(chip, core), :], local_sem.at[1]
        ),
        pltpu.make_async_copy(
            q_ref.at[:, cols(chip)], qq.at[query_rows(chip), 0:HEAD], local_sem.at[2]
        ),
        pltpu.make_async_copy(end_ref, ends.at[seq], local_sem.at[3]),
    ]
    for i in range(1, 2 * CHIPS):
        end_copy(i, (seq + i) % (2 * CHIPS)).start()
    for copy in own:
        copy.start()
    for b in range(1, CHIPS):
        q_copy(b).start()
    for b in range(1, CHIPS):
        k_copy(b).start()
        v_copy(b).start()
    own[0].wait()
    forward_k(0).start()
    own[1].wait()
    forward_v(0).start()

    loads = [
        pltpu.make_async_copy(g_ref.at[:, pl.ds(pl.multiple_of(core * half, half), half)], g_own, local_sem.at[4]),
        pltpu.make_async_copy(
            g_ref.at[:, pl.ds(pl.multiple_of((1 - core) * half, half), half)], g_sib, local_sem.at[5]
        ),
        pltpu.make_async_copy(w_ref, w_buf, local_sem.at[6]),
    ]
    for copy in loads:
        copy.start()
    vt[HEAD:, :] = jnp.ones((ONES, tokens), jnp.bfloat16)
    acc[...] = jnp.zeros_like(acc)
    top[...] = jnp.full_like(top, LOW)
    own[2].wait()
    own[3].wait()
    for i in range(1, 2 * CHIPS):
        end_copy(i, (seq + i) % (2 * CHIPS)).wait()

    every = ends[...].reshape(2 * CHIPS * 8, rows).astype(jnp.float32)

    def least(x):
        return jnp.min(jnp.min(x, axis=0, keepdims=True), axis=1, keepdims=True)

    whole = jnp.float32(tokens)
    first = least(every)
    second = least(jnp.where(every > first, every, whole))
    third = least(jnp.where(every > second, every, whole))
    lane = lax.broadcasted_iota(jnp.int32, (8, HEAD), 1)
    stop = jnp.where(lane == 0, first, jnp.where(lane == 1, second, jnp.where(lane == 2, third, whole)))
    start = jnp.where(
        lane == 0, jnp.float32(0), jnp.where(lane == 1, first, jnp.where(lane == 2, second, third))
    )
    start = jnp.where(lane < 4, start, 2.0 * whole)[0:1, :]
    stop = stop[0:1, :]

    def hide_keys(i, unused):
        base = pl.multiple_of(i * pair, pair)
        at = (base + lax.broadcasted_iota(jnp.int32, (pair, HEAD), 0)).astype(jnp.float32)
        kk[pl.ds(base, pair), HEAD:] = jnp.where(at >= stop, HIDE, 0.0).astype(jnp.bfloat16)
        return unused

    lax.fori_loop(0, CHIPS, hide_keys, 0)

    def mark_queries(i, unused):
        base = (i * 2 + core) * rows
        at = (base + lax.broadcasted_iota(jnp.int32, (rows, HEAD), 0)).astype(jnp.float32)
        inside = jnp.where(at >= start, 1.0, 0.0) * jnp.where(at < stop, 1.0, 0.0)
        qq[query_rows(i), HEAD:] = inside.astype(jnp.bfloat16)
        return unused

    lax.fori_loop(0, CHIPS, mark_queries, 0)
    for b in range(1, CHIPS):
        q_copy(b).wait_recv()

    def block_rows(b):
        return pl.ds(pl.multiple_of(chip_at(b, -1) * pair, pair), pair)

    def pass_on(b):
        k_copy(b).wait_recv()
        forward_k(b).start()
        v_copy(b).wait_recv()
        forward_v(b).start()

    def receive(b):
        forward_k(b).wait_recv()
        forward_v(b).wait_recv()
        at = block_rows(b)
        vt[0:HEAD, at] = vals[at, :].T

    def fill(b, step, u):
        queries = pl.ds(pl.multiple_of(step * WIDE, WIDE), WIDE)
        scores = lax.dot_general(
            kk[block_rows(b), :], qq[queries, :], (((1,), (1,)), ((), ())),
            preferred_element_type=jnp.float32,
        )
        sbuf_top[u, 0:1, :] = jnp.max(scores, axis=0, keepdims=True)
        sbuf[u] = scores

    def use(b, step, u):
        queries = pl.ds(pl.multiple_of(step * WIDE, WIDE), WIDE)
        old = top[0:1, queries]
        new = jnp.maximum(old, sbuf_top[u, 0:1, :])
        top[0:1, queries] = new
        weights = jnp.exp2(sbuf[u] * LOG2_SCALE - new * LOG2_SCALE).astype(jnp.bfloat16)
        factor = jnp.exp2((old - new) * LOG2_SCALE)
        product = jnp.dot(vt[:, block_rows(b)], weights, preferred_element_type=jnp.float32)
        acc[:, queries] = acc[:, queries] * factor + product

    receive(0)
    for u in range(GROUP):
        fill(0, u, u)

    def body(t, unused):
        b = t // steps
        i = t % steps

        @pl.when((i == steps - 2) & (b < CHIPS - 1))
        def _():
            pass_on(b + 1)

        @pl.when((i == steps - 1) & (b < CHIPS - 1))
        def _():
            receive(b + 1)

        later = jnp.minimum(t + 1, CHIPS * steps - 1)
        for u in range(GROUP):
            use(b, i * GROUP + u, u)
            fill(later // steps, (later % steps) * GROUP + u, u)
        return unused

    lax.fori_loop(0, CHIPS * steps, body, 0)

    def out_copy(b):
        to = chip_at(b, 1)
        return remote(
            obuf.at[query_rows(to), :], att.at[:, cols(chip)], o_send.at[b], o_recv.at[b], to, core
        )

    for b in (*range(1, CHIPS), 0):
        at = query_rows(chip_at(b, 1))
        result = (acc[0:HEAD, at] / acc[HEAD : HEAD + 1, at]).T.astype(jnp.bfloat16)
        if b:
            obuf[at, :] = result
            out_copy(b).start()
        else:
            att[:, cols(chip)] = result

    for b in range(1, CHIPS):
        q_copy(b).wait_send()
        k_copy(b).wait_send()
        v_copy(b).wait_send()
    for b in range(CHIPS):
        forward_k(b).wait_send()
        forward_v(b).wait_send()
    for copy in loads:
        copy.wait()

    def core_copy(b):
        head = chip_at(b, -1)
        return remote(
            part_sib.at[head], part_in.at[head], c_send.at[b], c_recv.at[b], chip, 1 - core
        )

    def share(b):
        head = chip_at(b, -1)
        turned = att[:, cols(head)].T
        part_sib[head] = jnp.dot(turned, g_sib[...], preferred_element_type=jnp.float32).astype(
            jnp.bfloat16
        )
        core_copy(b).start()
        part_own[head] = jnp.dot(turned, g_own[...], preferred_element_type=jnp.float32)

    share(0)

    def next_share(b, unused):
        out_copy(b).wait_recv()
        share(b)
        return unused

    lax.fori_loop(1, CHIPS, next_share, 0)

    def join_cores(b, unused):
        core_copy(b).wait_recv()
        head = chip_at(b, -1)
        both = part_own[head] + part_in[head].astype(jnp.float32)
        a0, a1 = PARTS[0], PARTS[0] + PARTS[1]
        tiles[0][0][head // 4, head % 4] = both[:, 0:a0].astype(jnp.bfloat16).reshape(8, 16, a0)
        tiles[1][0][head] = both[:, a0:a1].astype(jnp.bfloat16).reshape(4, 2, 16, a1 - a0)
        tiles[2][0][head // 4, pl.ds((head % 4) * 4, 4)] = (
            both[:, a1:].astype(jnp.bfloat16).reshape(4, 2, 16, half - a1)
        )
        return unused

    lax.fori_loop(0, CHIPS, join_cores, 0)

    def block(part, stage, d):
        tile = tiles[part][stage]
        axis = ORDERS[part][stage]
        if axis == "x":
            to = (x + d) % 4
            if part == 0:
                return tile.at[to % 2, to // 2]
            return tile.at[to % 2, :, to // 2]
        to = ((z if axis == "z" else row_y) + d) % 4
        if (part, stage) in ((0, 0), (0, 1), (1, 0)):
            return tile.at[:, to]
        return tile.at[to]

    def block_copy(part, stage, d):
        i = (part * 3 + stage) * 3 + d - 1
        return pltpu.make_async_remote_copy(
            src_ref=block(part, stage, d), dst_ref=landed[part][stage].at[d - 1],
            send_sem=r_send.at[i], recv_sem=r_recv.at[i],
            device_id=peer(ORDERS[part][stage], d), device_id_type=MESH,
        )

    def send(part, stage):
        for d in (1, 3, 2):
            block_copy(part, stage, d).start()

    def total(part, stage):
        for d in (1, 3, 2):
            block_copy(part, stage, d).wait_recv()
        value = block(part, stage, 0)[...].astype(jnp.float32)
        for d in range(3):
            value = value + landed[part][stage][d].astype(jnp.float32)
        return value

    for part in range(3):
        send(part, 0)

    def mix(i, unused):
        at = pl.ds(pl.multiple_of(i * 512, 512), 512)
        mixed[:, at] = jnp.dot(att[...], w_buf[:, at], preferred_element_type=jnp.float32).astype(
            jnp.bfloat16
        )
        return unused

    lax.fori_loop(0, w_buf.shape[1] // 512, mix, 0)
    mixed_copy = pltpu.make_async_copy(mixed, mixed_ref, s_sem.at[0])
    mixed_copy.start()

    for stage in range(2):
        for part in range(3):
            value = total(part, stage)
            tiles[part][stage + 1][...] = value.astype(jnp.bfloat16).reshape(
                tiles[part][stage + 1].shape
            )
            send(part, stage + 1)
    at = 0
    for part in range(3):
        value = total(part, 2)
        totals[0, :, at : at + PARTS[part]] = value[0:8]
        totals[1, :, at : at + PARTS[part]] = value[8:16]
        at += PARTS[part]
    own_columns = pl.ds(pl.multiple_of(core * half, half), half)
    last = pltpu.make_async_remote_copy(
        src_ref=totals.at[1 - core], dst_ref=grad.at[core], send_sem=s_sem.at[1],
        recv_sem=s_sem.at[2], device_id={"seq": chip * 2 + 1 - core}, device_id_type=MESH,
    )
    last.start()
    grad_own = pltpu.make_async_copy(totals.at[core], grad_ref.at[:, own_columns], s_sem.at[3])
    grad_own.start()
    last.wait()
    grad_other = pltpu.make_async_copy(
        grad.at[1 - core],
        grad_ref.at[:, pl.ds(pl.multiple_of((1 - core) * half, half), half)],
        s_sem.at[4],
    )
    grad_other.start()

    for b in range(1, CHIPS):
        out_copy(b).wait_send()
    for b in range(CHIPS):
        core_copy(b).wait_send()
    for part in range(3):
        for stage in range(3):
            for d in (1, 2, 3):
                block_copy(part, stage, d).wait_send()
    mixed_copy.wait()
    grad_own.wait()
    grad_other.wait()


def attend(q, k, v, ends, w, g):
    rows, width = q.shape
    out = w.shape[1]
    half = out // 2
    pair = 2 * rows
    tokens = CHIPS * pair
    mine = CHIPS * rows
    any_space = pl.BlockSpec(memory_space=pl.ANY)
    dma = pltpu.SemaphoreType.DMA
    bf16 = jnp.bfloat16
    p0, p1, p2 = PARTS
    tiles = (
        (
            pltpu.VMEM((2, 4, 8, 16, p0), bf16),
            pltpu.VMEM((2, 4, 2, 16, p0), bf16),
            pltpu.VMEM((2, 2, 16, p0), bf16),
        ),
        (
            pltpu.VMEM((8, 4, 2, 16, p1), bf16),
            pltpu.VMEM((2, 4, 2, 16, p1), bf16),
            pltpu.VMEM((4, 16, p1), bf16),
        ),
        (
            pltpu.VMEM((2, 16, 2, 16, p2), bf16),
            pltpu.VMEM((4, 4, 16, p2), bf16),
            pltpu.VMEM((4, 16, p2), bf16),
        ),
    )
    landed = (
        (
            pltpu.VMEM((3, 2, 8, 16, p0), bf16),
            pltpu.VMEM((3, 2, 2, 16, p0), bf16),
            pltpu.VMEM((3, 16, p0), bf16),
        ),
        (
            pltpu.VMEM((3, 8, 2, 16, p1), bf16),
            pltpu.VMEM((3, 4, 16, p1), bf16),
            pltpu.VMEM((3, 16, p1), bf16),
        ),
        (
            pltpu.VMEM((3, 16, 16, p2), bf16),
            pltpu.VMEM((3, 4, 16, p2), bf16),
            pltpu.VMEM((3, 16, p2), bf16),
        ),
    )
    return pl.pallas_call(
        functools.partial(attend_kernel, rows),
        out_shape=(
            jax.ShapeDtypeStruct((rows, out), bf16),
            jax.ShapeDtypeStruct((8, out), jnp.float32),
        ),
        in_specs=[any_space] * 6,
        out_specs=(any_space, any_space),
        scratch_shapes=[
            pltpu.VMEM((mine, 2 * HEAD), bf16),
            pltpu.VMEM((tokens, 2 * HEAD), bf16),
            pltpu.VMEM((tokens, HEAD), bf16),
            pltpu.VMEM((HEAD + ONES, tokens), bf16),
            pltpu.VMEM((2 * CHIPS, 8, rows), jnp.int32),
            pltpu.VMEM((HEAD + ONES, mine), jnp.float32),
            pltpu.VMEM((8, mine), jnp.float32),
            pltpu.VMEM((GROUP, pair, WIDE), jnp.float32),
            pltpu.VMEM((GROUP, 8, WIDE), jnp.float32),
            pltpu.VMEM((mine, HEAD), bf16),
            dma((7,)),
            dma((CHIPS,)), dma((CHIPS,)),
            dma((2, CHIPS)), dma((2, CHIPS)),
            dma((2, CHIPS)), dma((2, CHIPS)),
            dma((2 * CHIPS,)), dma((2 * CHIPS,)),
            dma((CHIPS,)), dma((CHIPS,)),
            pltpu.VMEM((rows, width), bf16),
            pltpu.VMEM((width, out), bf16),
            pltpu.VMEM((rows, half), bf16),
            pltpu.VMEM((rows, half), bf16),
            pltpu.VMEM((rows, out), bf16),
            pltpu.VMEM((CHIPS, HEAD, half), jnp.float32),
            pltpu.VMEM((CHIPS, HEAD, half), bf16),
            pltpu.VMEM((CHIPS, HEAD, half), bf16),
            tiles,
            landed,
            pltpu.VMEM((2, 8, half), jnp.float32),
            pltpu.VMEM((2, 8, half), jnp.float32),
            dma((CHIPS,)), dma((CHIPS,)),
            dma((27,)), dma((27,)),
            dma((5,)),
        ],
        compiler_params=pltpu.CompilerParams(
            collective_id=0, has_side_effects=True, vmem_limit_bytes=60 << 20
        ),
    )(q, k, v, ends, w, g)


def body(query_rows, key_rows, value_rows, scale_end, out_weight, grad_out):
    rows = query_rows.shape[1]
    ends = jnp.broadcast_to(scale_end[None, :], (8, rows))
    mixed_out, out_grad = attend(
        query_rows[0], key_rows[0], value_rows[0], ends, out_weight, grad_out[0]
    )
    return (mixed_out[None], out_grad)


def solution(mesh):
    torus = Mesh(mesh.devices.reshape(2, 4, mesh.shape["seq"]), ("dp_0", "dp_1", "seq"))
    in_specs = (
        P(DP, "seq", None),
        P(DP, "seq", None),
        P(DP, "seq", None),
        P("seq"),
        P(),
        P(DP, "seq", None),
    )
    out_specs = (P(DP, "seq", None), P(DP_SEQ, None))
    return jax.shard_map(body, mesh=torus, in_specs=in_specs, out_specs=out_specs, check_vma=False)
```

```python
import functools
import math

import jax
import jax.numpy as jnp
from jax import lax
from jax.experimental import pallas as pl
from jax.experimental.pallas import tpu as pltpu
from jax.sharding import Mesh
from jax.sharding import PartitionSpec as P

HEAD = 128
DP = ("dp_0", "dp_1")
PARTS = (384, 384, 256)
ORDERS = ("zyx", "yxz", "xzy")
DP_SEQ = ("dp_0", "dp_1", "seq")
MESH = pl.DeviceIdType.MESH
LOG2_SCALE = HEAD ** (-0.5) * math.log2(math.e)
LOW = -1e30
HIDE = -(2.0**100)
CHIPS = 8
WIDE = 256
GROUP = 3
ONES = 16


def attend_kernel(
    rows,
    q_ref, k_ref, v_ref, end_ref, w_ref, g_ref, mixed_ref, grad_ref,
    qq, kk, vals, vt, ends, acc, top, sbuf, sbuf_top, obuf,
    local_sem, q_send, q_recv, kv_send, kv_recv, f_send, f_recv, e_send, e_recv, o_send, o_recv,
    att, w_buf, g_own, g_sib, mixed, part_own, part_sib, part_in, tiles, landed, totals, grad,
    c_send, c_recv, r_send, r_recv, s_sem, z_send, z_recv, y_send, y_recv, x_send, x_recv,
):
    seq = lax.axis_index("seq")
    x_lo = lax.axis_index("dp_0")
    z = lax.axis_index("dp_1")
    half = g_own.shape[1]
    chip = seq // 2
    core = seq % 2
    row_y = chip // 2
    col_x = chip % 2
    pair = 2 * rows
    tokens = CHIPS * pair
    step_rows = GROUP * WIDE
    step_keys = 2 * pair

    def chip_at(b, sign):
        part = b // 2
        dy = part + part // 2 - 2 * (part // 3)
        return ((row_y + sign * dy + 4) % 4) * 2 + (col_x + b % 2) % 2

    barrier = pltpu.get_barrier_semaphore()
    for i in range(1, 2 * CHIPS):
        pl.semaphore_signal(
            barrier, inc=1, device_id={"seq": (seq + i) % (2 * CHIPS)}, device_id_type=MESH
        )
    x = col_x * 2 + x_lo

    def peer(axis, d):
        if axis == "z":
            return {"dp_1": (z + d) % 4}
        if axis == "y":
            return {"seq": ((row_y + d) % 4) * 4 + col_x * 2 + core}
        to = (x + d) % 4
        return {"dp_0": to % 2, "seq": row_y * 4 + (to // 2) * 2 + core}

    for axis, d in (("x", 1), ("x", 3), ("z", 1), ("z", 2), ("z", 3)):
        pl.semaphore_signal(barrier, inc=1, device_id=peer(axis, d), device_id_type=MESH)
    pl.semaphore_wait(barrier, 2 * CHIPS + 4)

    def cols(head):
        return pl.ds(pl.multiple_of(head * HEAD, HEAD), HEAD)

    def token_rows(b, j):
        return pl.ds(pl.multiple_of((b * 2 + j) * rows, rows), rows)

    def query_rows(b):
        return pl.ds(pl.multiple_of(b * rows, rows), rows)

    def remote(src, dst, send, recv, c, j):
        return pltpu.make_async_remote_copy(
            src_ref=src, dst_ref=dst, send_sem=send, recv_sem=recv,
            device_id={"seq": c * 2 + j}, device_id_type=MESH,
        )

    def end_copy(i, to):
        return pltpu.make_async_remote_copy(
            src_ref=end_ref, dst_ref=ends.at[seq], send_sem=e_send.at[i], recv_sem=e_recv.at[i],
            device_id={"seq": to}, device_id_type=MESH,
        )

    def q_copy(b):
        to = chip_at(b, 1)
        return remote(
            q_ref.at[:, cols(to)], qq.at[query_rows(b), 0:HEAD], q_send.at[b], q_recv.at[b], to, core
        )

    def k_copy(b):
        to = chip_at(b, 1)
        return remote(
            k_ref.at[:, cols(to)], kk.at[token_rows(b, core), 0:HEAD],
            kv_send.at[0, b], kv_recv.at[0, b], to, core,
        )

    def v_copy(b):
        to = chip_at(b, 1)
        return remote(
            v_ref.at[:, cols(to)], vals.at[token_rows(b, core), :],
            kv_send.at[1, b], kv_recv.at[1, b], to, core,
        )

    def forward_k(b):
        at = token_rows(b, core)
        return remote(
            kk.at[at, 0:HEAD], kk.at[at, 0:HEAD], f_send.at[0, b], f_recv.at[0, b], chip, 1 - core
        )

    def forward_v(b):
        at = token_rows(b, core)
        return remote(
            vals.at[at, :], vals.at[at, :], f_send.at[1, b], f_recv.at[1, b], chip, 1 - core
        )

    own = [
        pltpu.make_async_copy(
            k_ref.at[:, cols(chip)], kk.at[token_rows(0, core), 0:HEAD], local_sem.at[0]
        ),
        pltpu.make_async_copy(
            v_ref.at[:, cols(chip)], vals.at[token_rows(0, core), :], local_sem.at[1]
        ),
        pltpu.make_async_copy(
            q_ref.at[:, cols(chip)], qq.at[query_rows(0), 0:HEAD], local_sem.at[2]
        ),
        pltpu.make_async_copy(end_ref, ends.at[seq], local_sem.at[3]),
    ]
    for i in range(1, 2 * CHIPS):
        end_copy(i, (seq + i) % (2 * CHIPS)).start()
    for copy in own:
        copy.start()
    for queries, keys in (((1,), (1,)), ((2, 4, 3, 5), (2, 4, 3, 5)), ((6, 7), (6, 7))):
        for b in queries:
            q_copy(b).start()
        for b in keys:
            k_copy(b).start()
            v_copy(b).start()
    own[0].wait()
    forward_k(0).start()
    own[1].wait()
    forward_v(0).start()

    loads = [
        pltpu.make_async_copy(g_ref.at[:, pl.ds(pl.multiple_of(core * half, half), half)], g_own, local_sem.at[4]),
        pltpu.make_async_copy(
            g_ref.at[:, pl.ds(pl.multiple_of((1 - core) * half, half), half)], g_sib, local_sem.at[5]
        ),
        pltpu.make_async_copy(w_ref, w_buf, local_sem.at[6]),
    ]
    for copy in loads:
        copy.start()
    vt[HEAD:, :] = jnp.ones((ONES, tokens), jnp.bfloat16)
    acc[...] = jnp.zeros_like(acc)
    top[...] = jnp.full_like(top, LOW)
    own[2].wait()
    own[3].wait()
    for i in range(1, 2 * CHIPS):
        end_copy(i, (seq + i) % (2 * CHIPS)).wait()

    every = ends[...].reshape(2 * CHIPS * 8, rows).astype(jnp.float32)

    def least(x):
        return jnp.min(jnp.min(x, axis=0, keepdims=True), axis=1, keepdims=True)

    whole = jnp.float32(tokens)
    first = least(every)
    second = least(jnp.where(every > first, every, whole))
    third = least(jnp.where(every > second, every, whole))
    lane = lax.broadcasted_iota(jnp.int32, (8, HEAD), 1)
    stop = jnp.where(lane == 0, first, jnp.where(lane == 1, second, jnp.where(lane == 2, third, whole)))
    start = jnp.where(
        lane == 0, jnp.float32(0), jnp.where(lane == 1, first, jnp.where(lane == 2, second, third))
    )
    start = jnp.where(lane < 4, start, 2.0 * whole)[0:1, :]
    stop = stop[0:1, :]

    def hide_keys(b, unused):
        base = chip_at(b, -1) * pair
        at = (base + lax.broadcasted_iota(jnp.int32, (pair, HEAD), 0)).astype(jnp.float32)
        kk[pl.ds(pl.multiple_of(b * pair, pair), pair), HEAD:] = jnp.where(
            at >= stop, HIDE, 0.0
        ).astype(jnp.bfloat16)
        return unused

    lax.fori_loop(0, CHIPS, hide_keys, 0)

    def mark_queries(b, unused):
        base = (chip_at(b, -1) * 2 + core) * rows
        at = (base + lax.broadcasted_iota(jnp.int32, (rows, HEAD), 0)).astype(jnp.float32)
        inside = jnp.where(at >= start, 1.0, 0.0) * jnp.where(at < stop, 1.0, 0.0)
        qq[query_rows(b), HEAD:] = inside.astype(jnp.bfloat16)
        return unused

    lax.fori_loop(0, CHIPS, mark_queries, 0)

    def step_of(t):
        late, last = t // 9, t // 12
        p = (1 - late) * (t % 3) + late * 3 + last * (t % 4 - 3)
        n = (1 - late) * (t // 3) + (late - last) * (t % 3) + last * 3
        return p, n

    def key_rows(n):
        return pl.ds(pl.multiple_of(n * step_keys, step_keys), step_keys)

    def pass_on(b):
        k_copy(b).wait_recv()
        forward_k(b).start()
        v_copy(b).wait_recv()
        forward_v(b).start()

    def receive(n):
        for i in range(2):
            forward_k(2 * n + i).wait_recv()
            forward_v(2 * n + i).wait_recv()
        at = key_rows(n)
        vt[0:HEAD, at] = vals[at, :].T

    def fill(p, n, u):
        queries = pl.ds(pl.multiple_of(p * step_rows + u * WIDE, WIDE), WIDE)
        scores = lax.dot_general(
            kk[key_rows(n), :], qq[queries, :], (((1,), (1,)), ((), ())),
            preferred_element_type=jnp.float32,
        )
        sbuf_top[u, 0:1, :] = jnp.max(scores, axis=0, keepdims=True)
        sbuf[u] = scores

    def use(p, n, u):
        queries = pl.ds(pl.multiple_of(p * step_rows + u * WIDE, WIDE), WIDE)
        old = top[0:1, queries]
        new = jnp.maximum(old, sbuf_top[u, 0:1, :])
        top[0:1, queries] = new
        weights = jnp.exp2(sbuf[u] * LOG2_SCALE - new * LOG2_SCALE).astype(jnp.bfloat16)
        factor = jnp.exp2((old - new) * LOG2_SCALE)
        product = jnp.dot(vt[:, key_rows(n)], weights, preferred_element_type=jnp.float32)
        acc[:, queries] = acc[:, queries] * factor + product

    def out_copy(b):
        return remote(
            obuf.at[query_rows(b), :], att.at[:, cols(chip)], o_send.at[b], o_recv.at[b],
            chip_at(b, -1), core,
        )

    def result(b):
        at = query_rows(b)
        return (acc[0:HEAD, at] / acc[HEAD : HEAD + 1, at]).T.astype(jnp.bfloat16)

    pass_on(1)
    q_copy(1).wait_recv()
    receive(0)
    for u in range(GROUP):
        fill(0, 0, u)
    count = (CHIPS // 2) ** 2

    def body(t, unused):
        p, n = step_of(t)
        after = jnp.minimum(t + 1, count - 1)
        p1, n1 = step_of(after)

        @pl.when((t == 0) | (t == 1) | (t == 8))
        def _():
            q_copy(2 * p1).wait_recv()
            q_copy(2 * p1 + 1).wait_recv()

        @pl.when((t == 1) | (t == 4) | (t == 10))
        def _():
            n2 = n + 1 - t // 10 * (n - 2)
            pass_on(2 * n2)
            pass_on(2 * n2 + 1)

        @pl.when((t == 2) | (t == 5) | (t == 11))
        def _():
            receive(n1)

        for u in range(GROUP):
            use(p, n, u)
            fill(p1, n1, u)

        @pl.when(t == count - 4)
        def _():
            att[:, cols(chip)] = result(0)
            obuf[query_rows(1), :] = result(1)
            out_copy(1).start()

        @pl.when(t > count - 4)
        def _():
            for i in range(2):
                b = 2 * p + i
                obuf[query_rows(b), :] = result(b)
                out_copy(b).start()

        return unused

    lax.fori_loop(0, count, body, 0)
    for copy in loads:
        copy.wait()

    def core_copy(b):
        head = chip_at(b, 1)
        return remote(
            part_sib.at[head], part_in.at[head], c_send.at[b], c_recv.at[b], chip, 1 - core
        )

    def share(b):
        head = chip_at(b, 1)
        turned = att[:, cols(head)].T
        part_sib[head] = jnp.dot(turned, g_sib[...], preferred_element_type=jnp.float32).astype(
            jnp.bfloat16
        )
        core_copy(b).start()
        part_own[head] = jnp.dot(turned, g_own[...], preferred_element_type=jnp.float32)

    def z_copy(head, d):
        i = (d - 1) * 2 + head // 4
        return pltpu.make_async_remote_copy(
            src_ref=tiles[0][0].at[head // 4, head % 4], dst_ref=landed[0][0].at[d - 1, head // 4],
            send_sem=z_send.at[i], recv_sem=z_recv.at[i], device_id=peer("z", d), device_id_type=MESH,
        )

    def y_copy(head, d):
        i = (d - 1) * 8 + head
        return pltpu.make_async_remote_copy(
            src_ref=tiles[1][0].at[head, (row_y + d) % 4], dst_ref=landed[1][0].at[d - 1, head],
            send_sem=y_send.at[i], recv_sem=y_recv.at[i], device_id=peer("y", d), device_id_type=MESH,
        )

    def x_copy(hi, part, d):
        to = (x + d) % 4
        i = (d - 1) * 4 + hi
        at = pl.ds(hi * 4, 4)
        return pltpu.make_async_remote_copy(
            src_ref=tiles[2][0].at[part, at, to // 2], dst_ref=landed[2][0].at[d - 1, at],
            send_sem=x_send.at[i], recv_sem=x_recv.at[i], device_id=peer("x", d), device_id_type=MESH,
        )

    def join_cores(b):
        core_copy(b).wait_recv()
        head = chip_at(b, 1)
        both = part_own[head] + part_in[head].astype(jnp.float32)
        a0, a1 = PARTS[0], PARTS[0] + PARTS[1]
        lo, hi = head // 4, head % 4
        tiles[0][0][lo, hi] = both[:, 0:a0].astype(jnp.bfloat16).reshape(8, 16, a0)
        tiles[1][0][head] = both[:, a0:a1].astype(jnp.bfloat16).reshape(4, 2, 16, a1 - a0)
        tiles[2][0][lo, pl.ds(hi * 4, 4)] = (
            both[:, a1:].astype(jnp.bfloat16).reshape(4, 2, 16, half - a1)
        )
        dz = (hi - z + 4) % 4

        @pl.when(dz > 0)
        def _():
            z_copy(head, dz).start()

        for d in (1, 3, 2):
            y_copy(head, d).start()
        for to_hi in range(2):
            dx = (to_hi * 2 + lo - x + 4) % 4

            @pl.when(dx > 0)
            def _():
                x_copy(hi, lo, dx).start()

    share(0)

    def next_share(b, unused):
        out_copy(b).wait_recv()
        share(b)

        @pl.when(b > 1)
        def _():
            join_cores(b - 2)

        return unused

    lax.fori_loop(1, CHIPS, next_share, 0)
    join_cores(CHIPS - 2)
    join_cores(CHIPS - 1)

    def block(part, stage, d):
        tile = tiles[part][stage]
        axis = ORDERS[part][stage]
        if axis == "x":
            to = (x + d) % 4
            if part == 0:
                return tile.at[to % 2, to // 2]
            return tile.at[to % 2, :, to // 2]
        to = ((z if axis == "z" else row_y) + d) % 4
        if (part, stage) in ((0, 0), (0, 1), (1, 0)):
            return tile.at[:, to]
        return tile.at[to]

    def block_copy(part, stage, d):
        i = (part * 3 + stage) * 3 + d - 1
        return pltpu.make_async_remote_copy(
            src_ref=block(part, stage, d), dst_ref=landed[part][stage].at[d - 1],
            send_sem=r_send.at[i], recv_sem=r_recv.at[i],
            device_id=peer(ORDERS[part][stage], d), device_id_type=MESH,
        )

    def send(part, stage):
        for d in (1, 3, 2):
            block_copy(part, stage, d).start()

    def first_stage(part, d):
        if part == 0:
            return [z_copy(lo * 4 + (z + d) % 4, d) for lo in range(2)]
        if part == 1:
            return [y_copy(head, d) for head in range(CHIPS)]
        return [x_copy(hi, (x + d) % 2, d) for hi in range(4)]

    def total(part, stage):
        for d in (1, 3, 2):
            for copy in first_stage(part, d) if stage == 0 else [block_copy(part, stage, d)]:
                copy.wait_recv()
        value = block(part, stage, 0)[...].astype(jnp.float32)
        for d in range(3):
            value = value + landed[part][stage][d].astype(jnp.float32)
        return value

    def mix(i, unused):
        at = pl.ds(pl.multiple_of(i * 512, 512), 512)
        mixed[:, at] = jnp.dot(att[...], w_buf[:, at], preferred_element_type=jnp.float32).astype(
            jnp.bfloat16
        )
        return unused

    lax.fori_loop(0, w_buf.shape[1] // 512, mix, 0)
    mixed_copy = pltpu.make_async_copy(mixed, mixed_ref, s_sem.at[0])
    mixed_copy.start()

    for stage in range(2):
        for part in range(3):
            value = total(part, stage)
            tiles[part][stage + 1][...] = value.astype(jnp.bfloat16).reshape(
                tiles[part][stage + 1].shape
            )
            send(part, stage + 1)
    at = 0
    for part in range(3):
        value = total(part, 2)
        totals[0, :, at : at + PARTS[part]] = value[0:8]
        totals[1, :, at : at + PARTS[part]] = value[8:16]
        at += PARTS[part]
    own_columns = pl.ds(pl.multiple_of(core * half, half), half)
    last = pltpu.make_async_remote_copy(
        src_ref=totals.at[1 - core], dst_ref=grad.at[core], send_sem=s_sem.at[1],
        recv_sem=s_sem.at[2], device_id={"seq": chip * 2 + 1 - core}, device_id_type=MESH,
    )
    last.start()
    grad_own = pltpu.make_async_copy(totals.at[core], grad_ref.at[:, own_columns], s_sem.at[3])
    grad_own.start()
    last.wait()
    grad_other = pltpu.make_async_copy(
        grad.at[1 - core],
        grad_ref.at[:, pl.ds(pl.multiple_of((1 - core) * half, half), half)],
        s_sem.at[4],
    )
    grad_other.start()

    for b in range(1, CHIPS):
        out_copy(b).wait_send()
    for b in range(CHIPS):
        core_copy(b).wait_send()
    for part in range(3):
        for d in (1, 2, 3):
            for copy in first_stage(part, d):
                copy.wait_send()
            for stage in (1, 2):
                block_copy(part, stage, d).wait_send()
    for b in range(1, CHIPS):
        q_copy(b).wait_send()
        k_copy(b).wait_send()
        v_copy(b).wait_send()
    for b in range(CHIPS):
        forward_k(b).wait_send()
        forward_v(b).wait_send()
    mixed_copy.wait()
    grad_own.wait()
    grad_other.wait()


def attend(q, k, v, ends, w, g):
    rows, width = q.shape
    out = w.shape[1]
    half = out // 2
    pair = 2 * rows
    tokens = CHIPS * pair
    mine = CHIPS * rows
    any_space = pl.BlockSpec(memory_space=pl.ANY)
    dma = pltpu.SemaphoreType.DMA
    bf16 = jnp.bfloat16
    p0, p1, p2 = PARTS
    tiles = (
        (
            pltpu.VMEM((2, 4, 8, 16, p0), bf16),
            pltpu.VMEM((2, 4, 2, 16, p0), bf16),
            pltpu.VMEM((2, 2, 16, p0), bf16),
        ),
        (
            pltpu.VMEM((8, 4, 2, 16, p1), bf16),
            pltpu.VMEM((2, 4, 2, 16, p1), bf16),
            pltpu.VMEM((4, 16, p1), bf16),
        ),
        (
            pltpu.VMEM((2, 16, 2, 16, p2), bf16),
            pltpu.VMEM((4, 4, 16, p2), bf16),
            pltpu.VMEM((4, 16, p2), bf16),
        ),
    )
    landed = (
        (
            pltpu.VMEM((3, 2, 8, 16, p0), bf16),
            pltpu.VMEM((3, 2, 2, 16, p0), bf16),
            pltpu.VMEM((3, 16, p0), bf16),
        ),
        (
            pltpu.VMEM((3, 8, 2, 16, p1), bf16),
            pltpu.VMEM((3, 4, 16, p1), bf16),
            pltpu.VMEM((3, 16, p1), bf16),
        ),
        (
            pltpu.VMEM((3, 16, 16, p2), bf16),
            pltpu.VMEM((3, 4, 16, p2), bf16),
            pltpu.VMEM((3, 16, p2), bf16),
        ),
    )
    return pl.pallas_call(
        functools.partial(attend_kernel, rows),
        out_shape=(
            jax.ShapeDtypeStruct((rows, out), bf16),
            jax.ShapeDtypeStruct((8, out), jnp.float32),
        ),
        in_specs=[any_space] * 6,
        out_specs=(any_space, any_space),
        scratch_shapes=[
            pltpu.VMEM((mine, 2 * HEAD), bf16),
            pltpu.VMEM((tokens, 2 * HEAD), bf16),
            pltpu.VMEM((tokens, HEAD), bf16),
            pltpu.VMEM((HEAD + ONES, tokens), bf16),
            pltpu.VMEM((2 * CHIPS, 8, rows), jnp.int32),
            pltpu.VMEM((HEAD + ONES, mine), jnp.float32),
            pltpu.VMEM((8, mine), jnp.float32),
            pltpu.VMEM((GROUP, 2 * pair, WIDE), jnp.float32),
            pltpu.VMEM((GROUP, 8, WIDE), jnp.float32),
            pltpu.VMEM((mine, HEAD), bf16),
            dma((7,)),
            dma((CHIPS,)), dma((CHIPS,)),
            dma((2, CHIPS)), dma((2, CHIPS)),
            dma((2, CHIPS)), dma((2, CHIPS)),
            dma((2 * CHIPS,)), dma((2 * CHIPS,)),
            dma((CHIPS,)), dma((CHIPS,)),
            pltpu.VMEM((rows, width), bf16),
            pltpu.VMEM((width, out), bf16),
            pltpu.VMEM((rows, half), bf16),
            pltpu.VMEM((rows, half), bf16),
            pltpu.VMEM((rows, out), bf16),
            pltpu.VMEM((CHIPS, HEAD, half), jnp.float32),
            pltpu.VMEM((CHIPS, HEAD, half), bf16),
            pltpu.VMEM((CHIPS, HEAD, half), bf16),
            tiles,
            landed,
            pltpu.VMEM((2, 8, half), jnp.float32),
            pltpu.VMEM((2, 8, half), jnp.float32),
            dma((CHIPS,)), dma((CHIPS,)),
            dma((27,)), dma((27,)),
            dma((5,)),
            dma((6,)), dma((6,)),
            dma((24,)), dma((24,)),
            dma((12,)), dma((12,)),
        ],
        compiler_params=pltpu.CompilerParams(
            collective_id=0, has_side_effects=True, vmem_limit_bytes=60 << 20
        ),
    )(q, k, v, ends, w, g)


def body(query_rows, key_rows, value_rows, scale_end, out_weight, grad_out):
    rows = query_rows.shape[1]
    ends = jnp.broadcast_to(scale_end[None, :], (8, rows))
    mixed_out, out_grad = attend(
        query_rows[0], key_rows[0], value_rows[0], ends, out_weight, grad_out[0]
    )
    return (mixed_out[None], out_grad)


def solution(mesh):
    torus = Mesh(mesh.devices.reshape(2, 4, mesh.shape["seq"]), ("dp_0", "dp_1", "seq"))
    in_specs = (
        P(DP, "seq", None),
        P(DP, "seq", None),
        P(DP, "seq", None),
        P("seq"),
        P(),
        P(DP, "seq", None),
    )
    out_specs = (P(DP, "seq", None), P(DP_SEQ, None))
    return jax.shard_map(body, mesh=torus, in_specs=in_specs, out_specs=out_specs, check_vma=False)
```

```python
import functools
import math

import jax
import jax.numpy as jnp
from jax import lax
from jax.experimental import pallas as pl
from jax.experimental.pallas import tpu as pltpu
from jax.sharding import Mesh
from jax.sharding import PartitionSpec as P

HEAD = 128
DP = ("dp_0", "dp_1")
PARTS = (384, 384, 256)
ORDERS = ("zyx", "yxz", "xzy")
STEPS = (
    (0, 0), (1, 0), (2, 0), (0, 1), (1, 1), (2, 1), (3, 0), (3, 1),
    (0, 2), (1, 2), (2, 2), (3, 2), (3, 3), (2, 3), (1, 3), (0, 3),
)
HOME = (0, 6, 5, 2, 7, 1, 4, 3)
DP_SEQ = ("dp_0", "dp_1", "seq")
MESH = pl.DeviceIdType.MESH
LOG2_SCALE = HEAD ** (-0.5) * math.log2(math.e)
LOW = -1e30
HIDE = -(2.0**100)
CHIPS = 8
WIDE = 256
GROUP = 3
ONES = 16


def digits(values, base):
    return sum(value * base**i for i, value in enumerate(values))


def attend_kernel(
    rows,
    q_ref, k_ref, v_ref, end_ref, w_ref, g_ref, mixed_ref, grad,
    qq, kk, vals, vt, ends, acc, top, sbuf, sbuf_top, obuf,
    local_sem, q_recv, kv_recv, f_recv, o_recv, c_recv, e_recv, r_send, r_recv, sent,
    att, w_buf, g_own, g_sib, mixed, part_own, part_sib, part_in, tiles, landed,
):
    seq = lax.axis_index("seq")
    x_lo = lax.axis_index("dp_0")
    z = lax.axis_index("dp_1")
    half = g_own.shape[1]
    chip = seq // 2
    core = seq % 2
    row_y = chip // 2
    col_x = chip % 2
    pair = 2 * rows
    tokens = CHIPS * pair
    step_rows = GROUP * WIDE
    step_keys = 2 * pair

    def chip_at(b, sign):
        late, i = b // 4, b % 4
        dx = (1 - late) * (i // 3) + late * (1 - i % 2 * (1 - i // 3))
        dy = (1 - late) * (i % 3 + i % 3 // 2) + late * (i + 1 - 2 * (i // 3))
        return ((row_y + sign * dy + 4) % 4) * 2 + (col_x + dx) % 2

    barrier = pltpu.get_barrier_semaphore()
    for i in range(1, 2 * CHIPS):
        pl.semaphore_signal(
            barrier, inc=1, device_id={"seq": (seq + i) % (2 * CHIPS)}, device_id_type=MESH
        )
    x = col_x * 2 + x_lo

    def peer(axis, d):
        if axis == "z":
            return {"dp_1": (z + d) % 4}
        if axis == "y":
            return {"seq": ((row_y + d) % 4) * 4 + col_x * 2 + core}
        to = (x + d) % 4
        return {"dp_0": to % 2, "seq": row_y * 4 + (to // 2) * 2 + core}

    for axis, d in (("x", 1), ("x", 3), ("z", 1), ("z", 2), ("z", 3)):
        pl.semaphore_signal(barrier, inc=1, device_id=peer(axis, d), device_id_type=MESH)
    pl.semaphore_wait(barrier, 2 * CHIPS + 4)

    def cols(head):
        return pl.ds(pl.multiple_of(head * HEAD, HEAD), HEAD)

    def token_rows(b, j):
        return pl.ds(pl.multiple_of((b * 2 + j) * rows, rows), rows)

    def query_rows(b):
        return pl.ds(pl.multiple_of(b * rows, rows), rows)

    def remote(src, dst, send, recv, c, j):
        return pltpu.make_async_remote_copy(
            src_ref=src, dst_ref=dst, send_sem=send, recv_sem=recv,
            device_id={"seq": c * 2 + j}, device_id_type=MESH,
        )

    def settle(array, sem):
        pltpu.make_async_copy(array, array, sem).wait()

    def end_copy(to):
        return pltpu.make_async_remote_copy(
            src_ref=end_ref, dst_ref=ends.at[seq], send_sem=sent.at[0], recv_sem=e_recv.at[0],
            device_id={"seq": to}, device_id_type=MESH,
        )

    def send_queries(b):
        to = chip_at(b, 1)
        remote(
            q_ref.at[:, cols(to)], qq.at[query_rows(b), 0:HEAD], sent.at[1], q_recv.at[b // 2], to, core
        ).start()

    def send_keys(b):
        to = chip_at(b, 1)
        at = token_rows(b, core)
        remote(
            k_ref.at[:, cols(to)], kk.at[at, 0:HEAD], sent.at[2], kv_recv.at[b], to, core
        ).start()
        remote(v_ref.at[:, cols(to)], vals.at[at, :], sent.at[2], kv_recv.at[b], to, core).start()

    def forward(b):
        at = token_rows(b, core)
        remote(
            kk.at[at, 0:HEAD], kk.at[at, 0:HEAD], sent.at[3], f_recv.at[b // 2], chip, 1 - core
        ).start()
        remote(
            vals.at[at, :], vals.at[at, :], sent.at[3], f_recv.at[b // 2], chip, 1 - core
        ).start()

    own = [
        pltpu.make_async_copy(
            k_ref.at[:, cols(chip)], kk.at[token_rows(0, core), 0:HEAD], local_sem.at[0]
        ),
        pltpu.make_async_copy(
            v_ref.at[:, cols(chip)], vals.at[token_rows(0, core), :], local_sem.at[1]
        ),
        pltpu.make_async_copy(
            q_ref.at[:, cols(chip)], qq.at[query_rows(0), 0:HEAD], local_sem.at[2]
        ),
        pltpu.make_async_copy(end_ref, ends.at[seq], local_sem.at[3]),
    ]
    for i in range(1, 2 * CHIPS):
        end_copy((seq + i) % (2 * CHIPS)).start()
    for copy in own:
        copy.start()
    for b in (1, 2):
        send_queries(b)
        send_keys(b)
    send_queries(3)
    send_queries(4)
    send_keys(3)
    own[0].wait()
    own[1].wait()
    forward(0)

    loads = [
        pltpu.make_async_copy(g_ref.at[:, pl.ds(pl.multiple_of(core * half, half), half)], g_own, local_sem.at[4]),
        pltpu.make_async_copy(
            g_ref.at[:, pl.ds(pl.multiple_of((1 - core) * half, half), half)], g_sib, local_sem.at[5]
        ),
        pltpu.make_async_copy(w_ref, w_buf, local_sem.at[6]),
    ]
    for copy in loads:
        copy.start()
    vt[HEAD:, :] = jnp.ones((ONES, tokens), jnp.bfloat16)
    acc[...] = jnp.zeros_like(acc)
    top[...] = jnp.full_like(top, LOW)
    own[2].wait()
    own[3].wait()
    settle(ends.at[0 : 2 * CHIPS - 1], e_recv.at[0])

    every = ends[...].astype(jnp.float32)

    def least(x):
        return jnp.min(jnp.min(x, axis=0), axis=1, keepdims=True)

    whole = jnp.float32(tokens)
    first = least(every)
    second = least(jnp.where(every > first, every, whole))
    third = least(jnp.where(every > second, every, whole))
    lane = lax.broadcasted_iota(jnp.int32, (1, HEAD), 1)
    stop = jnp.where(lane == 0, first, jnp.where(lane == 1, second, jnp.where(lane == 2, third, whole)))
    start = jnp.where(
        lane == 0, jnp.float32(0), jnp.where(lane == 1, first, jnp.where(lane == 2, second, third))
    )
    start = jnp.where(lane < 4, start, 2.0 * whole)

    def hide_keys(b, unused):
        base = chip_at(b, -1) * pair
        at = (base + lax.broadcasted_iota(jnp.int32, (pair, HEAD), 0)).astype(jnp.float32)
        kk[pl.ds(pl.multiple_of(b * pair, pair), pair), HEAD:] = jnp.where(
            at >= stop, HIDE, 0.0
        ).astype(jnp.bfloat16)
        return unused

    lax.fori_loop(0, CHIPS, hide_keys, 0)

    def mark_queries(b, unused):
        base = (chip_at(b, -1) * 2 + core) * rows
        at = (base + lax.broadcasted_iota(jnp.int32, (rows, HEAD), 0)).astype(jnp.float32)
        inside = jnp.where(at >= start, 1.0, 0.0) * jnp.where(at < stop, 1.0, 0.0)
        qq[query_rows(b), HEAD:] = inside.astype(jnp.bfloat16)
        return unused

    lax.fori_loop(0, CHIPS, mark_queries, 0)

    send_queries(5)
    send_keys(4)
    send_keys(5)
    send_queries(6)
    send_queries(7)
    send_keys(6)
    send_keys(7)

    half_steps = len(STEPS) // 2

    def step_of(t, power):
        late = t // half_steps
        first = [digits([step[i] for step in STEPS[:half_steps]], 4) for i in range(2)]
        second = [digits([step[i] for step in STEPS[half_steps:]], 4) for i in range(2)]
        return [(a + late * (b - a)) // power % 4 for a, b in zip(first, second)]

    def key_rows(n):
        return pl.ds(pl.multiple_of(n * step_keys, step_keys), step_keys)

    def pass_on(b):
        settle(kk.at[0:pair, 0:HEAD], kv_recv.at[b])
        forward(b)

    def receive(n):
        settle(kk.at[0:step_keys, 0:HEAD], f_recv.at[n])
        at = key_rows(n)
        vt[0:HEAD, at] = vals[at, :].T

    def fill(p, n, u):
        queries = pl.ds(pl.multiple_of(p * step_rows + u * WIDE, WIDE), WIDE)
        scores = lax.dot_general(
            kk[key_rows(n), :], qq[queries, :], (((1,), (1,)), ((), ())),
            preferred_element_type=jnp.float32,
        )
        sbuf_top[u, 0:1, :] = jnp.max(scores, axis=0, keepdims=True)
        sbuf[u] = scores

    def use(p, n, u):
        queries = pl.ds(pl.multiple_of(p * step_rows + u * WIDE, WIDE), WIDE)
        old = top[0:1, queries]
        new = jnp.maximum(old, sbuf_top[u, 0:1, :])
        top[0:1, queries] = new
        weights = jnp.exp2(sbuf[u] * LOG2_SCALE - new * LOG2_SCALE).astype(jnp.bfloat16)
        factor = jnp.exp2((old - new) * LOG2_SCALE)
        product = jnp.dot(vt[:, key_rows(n)], weights, preferred_element_type=jnp.float32)
        acc[:, queries] = acc[:, queries] * factor + product

    def out_copy(b):
        return remote(
            obuf.at[query_rows(b), :], att.at[:, cols(chip)], sent.at[4], o_recv.at[b],
            chip_at(b, -1), core,
        )

    def result(b):
        at = query_rows(b)
        return (acc[0:HEAD, at] / acc[HEAD : HEAD + 1, at]).T.astype(jnp.bfloat16)

    settle(qq.at[0:rows, 0:HEAD], q_recv.at[0])
    pass_on(1)
    receive(0)
    for u in range(GROUP):
        fill(0, 0, u)
    count = len(STEPS)

    def body(t, power):
        p, n = step_of(t, power)
        after = jnp.minimum(t + 1, count - 1)
        wrap = t % half_steps // (half_steps - 1)
        power_after = power * 4 * (1 - wrap) + wrap
        p1, n1 = step_of(after, power_after)

        @pl.when((t < 2) | (t == 5))
        def _():
            settle(qq.at[0:pair, 0:HEAD], q_recv.at[p1])

        @pl.when((t == 1) | (t == 6) | (t == 10))
        def _():
            n2 = (t + 3) // 4
            pass_on(2 * n2)
            pass_on(2 * n2 + 1)

        @pl.when((t == 2) | (t == 7) | (t == 11))
        def _():
            receive(n1)

        for u in range(GROUP):
            use(p, n, u)
            fill(p1, n1, u)

        @pl.when((t > 11) & (t < 15))
        def _():
            for i in range(2):
                b = 2 * p + i
                obuf[query_rows(b), :] = result(b)
                out_copy(b).start()

        @pl.when(t == 15)
        def _():
            obuf[query_rows(1), :] = result(1)
            out_copy(1).start()
            att[:, cols(chip)] = result(0)

        return power_after

    lax.fori_loop(0, count, body, 1)
    for copy in loads:
        copy.wait()

    def core_copy(b):
        head = chip_at(b, 1)
        return remote(
            part_sib.at[head], part_in.at[head], sent.at[5], c_recv.at[b], chip, 1 - core
        )

    def share(b):
        head = chip_at(b, 1)
        turned = att[:, cols(head)].T
        part_sib[head] = jnp.dot(turned, g_sib[...], preferred_element_type=jnp.float32).astype(
            jnp.bfloat16
        )
        core_copy(b).start()
        part_own[head] = jnp.dot(turned, g_own[...], preferred_element_type=jnp.float32)

    def z_copy(head, d):
        return pltpu.make_async_remote_copy(
            src_ref=tiles[0][0].at[head // 4, head % 4], dst_ref=landed[0][0].at[d - 1, head // 4],
            send_sem=r_send.at[0, 0], recv_sem=r_recv.at[0, 0], device_id=peer("z", d), device_id_type=MESH,
        )

    def y_copy(head, d):
        return pltpu.make_async_remote_copy(
            src_ref=tiles[1][0].at[head, (row_y + d) % 4], dst_ref=landed[1][0].at[d - 1, head],
            send_sem=r_send.at[1, 0], recv_sem=r_recv.at[1, 0], device_id=peer("y", d), device_id_type=MESH,
        )

    def x_copy(hi, part, d):
        to = (x + d) % 4
        at = pl.ds(hi * 4, 4)
        return pltpu.make_async_remote_copy(
            src_ref=tiles[2][0].at[part, at, to // 2], dst_ref=landed[2][0].at[d - 1, at],
            send_sem=r_send.at[2, 0], recv_sem=r_recv.at[2, 0], device_id=peer("x", d), device_id_type=MESH,
        )

    def join_cores(b):
        core_copy(b).wait_recv()
        head = chip_at(b, 1)
        both = part_own[head] + part_in[head].astype(jnp.float32)
        a0, a1 = PARTS[0], PARTS[0] + PARTS[1]
        lo, hi = head // 4, head % 4
        tiles[0][0][lo, hi] = both[:, 0:a0].astype(jnp.bfloat16).reshape(8, 16, a0)
        tiles[1][0][head] = both[:, a0:a1].astype(jnp.bfloat16).reshape(4, 2, 16, a1 - a0)
        tiles[2][0][lo, pl.ds(hi * 4, 4)] = (
            both[:, a1:].astype(jnp.bfloat16).reshape(4, 2, 16, half - a1)
        )
        dz = (hi - z + 4) % 4

        @pl.when(dz > 0)
        def _():
            z_copy(head, dz).start()

        for d in (1, 3, 2):
            y_copy(head, d).start()
        for to_hi in range(2):
            dx = (to_hi * 2 + lo - x + 4) % 4

            @pl.when(dx > 0)
            def _():
                x_copy(hi, lo, dx).start()

    share(0)
    order = digits(HOME, CHIPS)

    def next_share(i, power):
        b = order // power % CHIPS
        out_copy(b).wait_recv()
        share(b)

        @pl.when(i > 1)
        def _():
            join_cores(order // (power // (CHIPS * CHIPS)) % CHIPS)

        return power * CHIPS

    lax.fori_loop(1, CHIPS, next_share, CHIPS)
    join_cores(HOME[-2])
    join_cores(HOME[-1])

    def block(part, stage, d):
        tile = tiles[part][stage]
        axis = ORDERS[part][stage]
        if axis == "x":
            to = (x + d) % 4
            if part == 0:
                return tile.at[to % 2, to // 2]
            return tile.at[to % 2, :, to // 2]
        to = ((z if axis == "z" else row_y) + d) % 4
        if (part, stage) in ((0, 0), (0, 1), (1, 0)):
            return tile.at[:, to]
        return tile.at[to]

    def block_copy(part, stage, d):
        return pltpu.make_async_remote_copy(
            src_ref=block(part, stage, d), dst_ref=landed[part][stage].at[d - 1],
            send_sem=r_send.at[part, stage], recv_sem=r_recv.at[part, stage],
            device_id=peer(ORDERS[part][stage], d), device_id_type=MESH,
        )

    def send(part, stage):
        for d in (1, 3, 2):
            block_copy(part, stage, d).start()

    def total(part, stage):
        settle(landed[part][stage], r_recv.at[part, stage])
        value = block(part, stage, 0)[...].astype(jnp.float32)
        for d in range(3):
            value = value + landed[part][stage][d].astype(jnp.float32)
        return value

    def mix(i, unused):
        at = pl.ds(pl.multiple_of(i * 512, 512), 512)
        mixed[:, at] = jnp.dot(att[...], w_buf[:, at], preferred_element_type=jnp.float32).astype(
            jnp.bfloat16
        )
        return unused

    lax.fori_loop(0, w_buf.shape[1] // 512, mix, 0)
    mixed_copy = pltpu.make_async_copy(mixed, mixed_ref, local_sem.at[7])
    mixed_copy.start()

    for part in range(3):
        tiles[part][1][...] = total(part, 0).astype(jnp.bfloat16).reshape(tiles[part][1].shape)
        send(part, 1)

    def last_copies(part):
        copies = []
        for d in (0, 1, 3, 2):
            for other in range(2):
                if d or other:
                    slot = 3 + d if other else d - 1
                    to = (core + other) % 2
                    target = dict(peer(ORDERS[part][2], d))
                    target["seq"] = target.get("seq", seq) + to - core
                    copies.append(
                        pltpu.make_async_remote_copy(
                            src_ref=block(part, 2, d).at[to], dst_ref=landed[part][2].at[slot],
                            send_sem=r_send.at[part, 2], recv_sem=r_recv.at[part, 2],
                            device_id=target, device_id_type=MESH,
                        )
                    )
        return copies

    for part in range(3):
        tiles[part][2][...] = total(part, 1).reshape(tiles[part][2].shape)
        for copy in last_copies(part):
            copy.start()
    at = 0
    for part in range(3):
        settle(landed[part][2], r_recv.at[part, 2])
        ours = block(part, 2, 0).at[core][...]
        for d in range(3):
            ours = ours + landed[part][2][d]
        theirs = landed[part][2][3]
        for d in range(4, 7):
            theirs = theirs + landed[part][2][d]
        grad[:, pl.ds(pl.multiple_of(core * half + at, HEAD), PARTS[part])] = ours
        grad[:, pl.ds(pl.multiple_of((1 - core) * half + at, HEAD), PARTS[part])] = theirs
        at += PARTS[part]

    mixed_copy.wait()
    some = (CHIPS - 1) * rows
    settle(ends.at[0 : 2 * CHIPS - 1], sent.at[0])
    settle(qq.at[0:some, 0:HEAD], sent.at[1])
    settle(kk.at[0 : 2 * some, 0:HEAD], sent.at[2])
    settle(kk.at[:, 0:HEAD], sent.at[3])
    settle(obuf.at[0:some, :], sent.at[4])
    settle(part_sib, sent.at[5])
    for part in range(3):
        for stage in range(3):
            settle(landed[part][stage], r_send.at[part, stage])


def attend(q, k, v, ends, w, g):
    rows, width = q.shape
    out = w.shape[1]
    half = out // 2
    pair = 2 * rows
    tokens = CHIPS * pair
    mine = CHIPS * rows
    dma = pltpu.SemaphoreType.DMA
    bf16 = jnp.bfloat16
    p0, p1, p2 = PARTS
    tiles = (
        (
            pltpu.VMEM((2, 4, 8, 16, p0), bf16),
            pltpu.VMEM((2, 4, 2, 16, p0), bf16),
            pltpu.VMEM((2, 2, 2, 8, p0), jnp.float32),
        ),
        (
            pltpu.VMEM((8, 4, 2, 16, p1), bf16),
            pltpu.VMEM((2, 4, 2, 16, p1), bf16),
            pltpu.VMEM((4, 2, 8, p1), jnp.float32),
        ),
        (
            pltpu.VMEM((2, 16, 2, 16, p2), bf16),
            pltpu.VMEM((4, 4, 16, p2), bf16),
            pltpu.VMEM((4, 2, 8, p2), jnp.float32),
        ),
    )
    landed = (
        (
            pltpu.VMEM((3, 2, 8, 16, p0), bf16),
            pltpu.VMEM((3, 2, 2, 16, p0), bf16),
            pltpu.VMEM((7, 8, p0), jnp.float32),
        ),
        (
            pltpu.VMEM((3, 8, 2, 16, p1), bf16),
            pltpu.VMEM((3, 4, 16, p1), bf16),
            pltpu.VMEM((7, 8, p1), jnp.float32),
        ),
        (
            pltpu.VMEM((3, 16, 16, p2), bf16),
            pltpu.VMEM((3, 4, 16, p2), bf16),
            pltpu.VMEM((7, 8, p2), jnp.float32),
        ),
    )
    return pl.pallas_call(
        functools.partial(attend_kernel, rows),
        out_shape=(
            jax.ShapeDtypeStruct((rows, out), bf16),
            jax.ShapeDtypeStruct((8, out), jnp.float32),
        ),
        in_specs=[pl.BlockSpec(memory_space=pl.ANY)] * 6,
        out_specs=(pl.BlockSpec(memory_space=pl.ANY), pl.BlockSpec(memory_space=pltpu.VMEM)),
        scratch_shapes=[
            pltpu.VMEM((mine, 2 * HEAD), bf16),
            pltpu.VMEM((tokens, 2 * HEAD), bf16),
            pltpu.VMEM((tokens, HEAD), bf16),
            pltpu.VMEM((HEAD + ONES, tokens), bf16),
            pltpu.VMEM((2 * CHIPS, 1, rows), jnp.int32),
            pltpu.VMEM((HEAD + ONES, mine), jnp.float32),
            pltpu.VMEM((8, mine), jnp.float32),
            pltpu.VMEM((GROUP, 2 * pair, WIDE), jnp.float32),
            pltpu.VMEM((GROUP, 8, WIDE), jnp.float32),
            pltpu.VMEM((mine, HEAD), bf16),
            dma((8,)),
            dma((4,)), dma((CHIPS,)), dma((4,)), dma((CHIPS,)), dma((CHIPS,)), dma((1,)),
            dma((3, 3)), dma((3, 3)), dma((6,)),
            pltpu.VMEM((rows, width), bf16),
            pltpu.VMEM((width, out), bf16),
            pltpu.VMEM((rows, half), bf16),
            pltpu.VMEM((rows, half), bf16),
            pltpu.VMEM((rows, out), bf16),
            pltpu.VMEM((CHIPS, HEAD, half), jnp.float32),
            pltpu.VMEM((CHIPS, HEAD, half), bf16),
            pltpu.VMEM((CHIPS, HEAD, half), bf16),
            tiles,
            landed,
        ],
        compiler_params=pltpu.CompilerParams(
            collective_id=0, has_side_effects=True, vmem_limit_bytes=60 << 20
        ),
    )(q, k, v, ends, w, g)


def body(query_rows, key_rows, value_rows, scale_end, out_weight, grad_out):
    rows = query_rows.shape[1]
    ends = scale_end.reshape(1, rows)
    mixed_out, out_grad = attend(
        query_rows[0], key_rows[0], value_rows[0], ends, out_weight, grad_out[0]
    )
    return (mixed_out[None], out_grad)


def solution(mesh):
    torus = Mesh(mesh.devices.reshape(2, 4, mesh.shape["seq"]), ("dp_0", "dp_1", "seq"))
    in_specs = (
        P(DP, "seq", None),
        P(DP, "seq", None),
        P(DP, "seq", None),
        P("seq"),
        P(),
        P(DP, "seq", None),
    )
    out_specs = (P(DP, "seq", None), P(DP_SEQ, None))
    return jax.shard_map(body, mesh=torus, in_specs=in_specs, out_specs=out_specs, check_vma=False)
```

```python
import functools
import math

import jax
import jax.numpy as jnp
from jax import lax
from jax.experimental import pallas as pl
from jax.experimental.pallas import tpu as pltpu
from jax.sharding import Mesh
from jax.sharding import PartitionSpec as P

HEAD = 128
DP = ("dp_0", "dp_1")
PARTS = (384, 384, 256)
ORDERS = ("zyx", "yxz", "xzy")
FIRST = (2, 1, 0)
STEPS = (
    (0, 0), (1, 0), (2, 0), (0, 1), (1, 1), (2, 1), (3, 0), (3, 1),
    (3, 2), (2, 2), (1, 2), (3, 3), (2, 3), (1, 3), (0, 2), (0, 3),
)
HOME = ((0, 6), (7, 5), (4, 2), (3, 1))
DP_SEQ = ("dp_0", "dp_1", "seq")
MESH = pl.DeviceIdType.MESH
LOG2_SCALE = HEAD ** (-0.5) * math.log2(math.e)
LOW = -1e30
HIDE = -(2.0**100)
CHIPS = 8
PIECES = 4
WIDE = 256
GROUP = 3
ONES = 16


def digits(values, base):
    return sum(value * base**i for i, value in enumerate(values))


def attend_kernel(
    rows,
    q_ref, k_ref, v_ref, end_ref, w_ref, g_ref, mixed_ref, grad,
    qq, kk, vals, vt, ends, acc, top, sbuf, sbuf_top, obuf,
    local_sem, q_recv, kv_recv, f_recv, o_recv, c_recv, e_recv, r_send, r_recv, sent,
    att, w_buf, g_own, g_sib, mixed, part_own, part_sib, part_in, tiles, landed,
):
    seq = lax.axis_index("seq")
    x_lo = lax.axis_index("dp_0")
    z = lax.axis_index("dp_1")
    half = g_own.shape[1]
    chip = seq // 2
    core = seq % 2
    row_y = chip // 2
    col_x = chip % 2
    pair = 2 * rows
    tokens = CHIPS * pair
    step_rows = GROUP * WIDE
    step_keys = 2 * pair

    def chip_at(b, sign):
        late, i = b // 4, b % 4
        dx = (1 - late) * (i // 3) + late * (1 - i % 2 * (1 - i // 3))
        dy = (1 - late) * (i % 3 + i % 3 // 2) + late * (i + 1 - 2 * (i // 3))
        return ((row_y + sign * dy + 4) % 4) * 2 + (col_x + dx) % 2

    barrier = pltpu.get_barrier_semaphore()
    for i in range(1, 2 * CHIPS):
        pl.semaphore_signal(
            barrier, inc=1, device_id={"seq": (seq + i) % (2 * CHIPS)}, device_id_type=MESH
        )
    x = col_x * 2 + x_lo

    def peer(axis, d):
        if axis == "z":
            return {"dp_1": (z + d) % 4}
        if axis == "y":
            return {"seq": ((row_y + d) % 4) * 4 + col_x * 2 + core}
        to = (x + d) % 4
        return {"dp_0": to % 2, "seq": row_y * 4 + (to // 2) * 2 + core}

    for axis, d in (("x", 1), ("x", 3), ("z", 1), ("z", 2), ("z", 3)):
        pl.semaphore_signal(barrier, inc=1, device_id=peer(axis, d), device_id_type=MESH)
    pl.semaphore_wait(barrier, 2 * CHIPS + 4)

    def cols(head):
        return pl.ds(pl.multiple_of(head * HEAD, HEAD), HEAD)

    def token_rows(b, j):
        return pl.ds(pl.multiple_of((b * 2 + j) * rows, rows), rows)

    def query_rows(b):
        return pl.ds(pl.multiple_of(b * rows, rows), rows)

    def remote(src, dst, send, recv, c, j):
        return pltpu.make_async_remote_copy(
            src_ref=src, dst_ref=dst, send_sem=send, recv_sem=recv,
            device_id={"seq": c * 2 + j}, device_id_type=MESH,
        )

    def settle(array, sem):
        pltpu.make_async_copy(array, array, sem).wait()

    def end_copy(to):
        return pltpu.make_async_remote_copy(
            src_ref=end_ref, dst_ref=ends.at[seq, 0], send_sem=sent.at[0], recv_sem=e_recv.at[0],
            device_id={"seq": to}, device_id_type=MESH,
        )

    def send_queries(b):
        to = chip_at(b, 1)
        remote(
            q_ref.at[:, cols(to)], qq.at[query_rows(b), 0:HEAD], sent.at[1], q_recv.at[b // 2], to, core
        ).start()

    def send_keys(b):
        to = chip_at(b, 1)
        at = token_rows(b, core)
        remote(
            k_ref.at[:, cols(to)], kk.at[at, 0:HEAD], sent.at[2], kv_recv.at[b], to, core
        ).start()
        remote(v_ref.at[:, cols(to)], vals.at[at, :], sent.at[2], kv_recv.at[b], to, core).start()

    def forward(b):
        at = token_rows(b, core)
        remote(
            kk.at[at, 0:HEAD], kk.at[at, 0:HEAD], sent.at[3], f_recv.at[b // 2], chip, 1 - core
        ).start()
        remote(
            vals.at[at, :], vals.at[at, :], sent.at[3], f_recv.at[b // 2], chip, 1 - core
        ).start()

    own = [
        pltpu.make_async_copy(
            k_ref.at[:, cols(chip)], kk.at[token_rows(0, core), 0:HEAD], local_sem.at[0]
        ),
        pltpu.make_async_copy(
            v_ref.at[:, cols(chip)], vals.at[token_rows(0, core), :], local_sem.at[1]
        ),
        pltpu.make_async_copy(
            q_ref.at[:, cols(chip)], qq.at[query_rows(0), 0:HEAD], local_sem.at[2]
        ),
        pltpu.make_async_copy(end_ref, ends.at[seq, 0], local_sem.at[3]),
    ]
    for i in range(1, 2 * CHIPS):
        end_copy((seq + i) % (2 * CHIPS)).start()
    for copy in own:
        copy.start()
    for b in (1, 2):
        send_queries(b)
        send_keys(b)
    send_queries(3)
    send_queries(4)
    send_keys(3)
    own[0].wait()
    own[1].wait()
    forward(0)

    loads = [
        pltpu.make_async_copy(g_ref.at[:, pl.ds(pl.multiple_of(core * half, half), half)], g_own, local_sem.at[4]),
        pltpu.make_async_copy(
            g_ref.at[:, pl.ds(pl.multiple_of((1 - core) * half, half), half)], g_sib, local_sem.at[5]
        ),
        pltpu.make_async_copy(w_ref, w_buf, local_sem.at[6]),
    ]
    for copy in loads:
        copy.start()
    vt[HEAD:, :] = jnp.ones((ONES, tokens), jnp.bfloat16)
    acc[...] = jnp.zeros_like(acc)
    top[...] = jnp.full_like(top, LOW)
    own[2].wait()
    own[3].wait()
    settle(ends.at[0 : 2 * CHIPS - 1], e_recv.at[0])

    every = ends[...].astype(jnp.float32)

    def least(x):
        return jnp.min(jnp.min(x, axis=0), axis=1, keepdims=True)

    whole = jnp.float32(tokens)
    first = least(every)
    second = least(jnp.where(every > first, every, whole))
    third = least(jnp.where(every > second, every, whole))
    lane = lax.broadcasted_iota(jnp.int32, (1, HEAD), 1)
    stop = jnp.where(lane == 0, first, jnp.where(lane == 1, second, jnp.where(lane == 2, third, whole)))
    start = jnp.where(
        lane == 0, jnp.float32(0), jnp.where(lane == 1, first, jnp.where(lane == 2, second, third))
    )
    start = jnp.where(lane < 4, start, 2.0 * whole)

    def hide_keys(b, unused):
        base = chip_at(b, -1) * pair
        at = (base + lax.broadcasted_iota(jnp.int32, (pair, HEAD), 0)).astype(jnp.float32)
        kk[pl.ds(pl.multiple_of(b * pair, pair), pair), HEAD:] = jnp.where(
            at >= stop, HIDE, 0.0
        ).astype(jnp.bfloat16)
        return unused

    lax.fori_loop(0, CHIPS, hide_keys, 0)

    def mark_queries(b, unused):
        base = (chip_at(b, -1) * 2 + core) * rows
        at = (base + lax.broadcasted_iota(jnp.int32, (rows, HEAD), 0)).astype(jnp.float32)
        inside = jnp.where(at >= start, 1.0, 0.0) * jnp.where(at < stop, 1.0, 0.0)
        qq[query_rows(b), HEAD:] = inside.astype(jnp.bfloat16)
        return unused

    lax.fori_loop(0, CHIPS, mark_queries, 0)

    send_queries(5)
    send_keys(4)
    send_keys(5)
    send_queries(6)
    send_queries(7)
    send_keys(6)
    send_keys(7)

    half_steps = len(STEPS) // 2

    def step_of(t, power):
        late = t // half_steps
        first = [digits([step[i] for step in STEPS[:half_steps]], 4) for i in range(2)]
        second = [digits([step[i] for step in STEPS[half_steps:]], 4) for i in range(2)]
        return [(a + late * (b - a)) // power % 4 for a, b in zip(first, second)]

    def key_rows(n):
        return pl.ds(pl.multiple_of(n * step_keys, step_keys), step_keys)

    def pass_on(b):
        settle(kk.at[0:pair, 0:HEAD], kv_recv.at[b])
        forward(b)

    def receive(n):
        settle(kk.at[0:step_keys, 0:HEAD], f_recv.at[n])
        at = key_rows(n)
        vt[0:HEAD, at] = vals[at, :].T

    def fill(p, n, u):
        queries = pl.ds(pl.multiple_of(p * step_rows + u * WIDE, WIDE), WIDE)
        scores = lax.dot_general(
            kk[key_rows(n), :], qq[queries, :], (((1,), (1,)), ((), ())),
            preferred_element_type=jnp.float32,
        )
        sbuf_top[u, 0:1, :] = jnp.max(scores, axis=0, keepdims=True)
        sbuf[u] = scores

    def use(p, n, u):
        queries = pl.ds(pl.multiple_of(p * step_rows + u * WIDE, WIDE), WIDE)
        old = top[0:1, queries]
        new = jnp.maximum(old, sbuf_top[u, 0:1, :])
        top[0:1, queries] = new
        weights = jnp.exp2(sbuf[u] * LOG2_SCALE - new * LOG2_SCALE).astype(jnp.bfloat16)
        factor = jnp.exp2((old - new) * LOG2_SCALE)
        product = jnp.dot(vt[:, key_rows(n)], weights, preferred_element_type=jnp.float32)
        acc[:, queries] = acc[:, queries] * factor + product

    def out_copy(b):
        return remote(
            obuf.at[query_rows(b), :], att.at[:, cols(chip)], sent.at[4], o_recv.at[b],
            chip_at(b, -1), core,
        )

    def result(b):
        at = query_rows(b)
        return (acc[0:HEAD, at] / acc[HEAD : HEAD + 1, at]).T.astype(jnp.bfloat16)

    settle(qq.at[0:rows, 0:HEAD], q_recv.at[0])
    pass_on(1)
    receive(0)
    for u in range(GROUP):
        fill(0, 0, u)
    count = len(STEPS)

    def body(t, power):
        p, n = step_of(t, power)
        after = jnp.minimum(t + 1, count - 1)
        wrap = t % half_steps // (half_steps - 1)
        power_after = power * 4 * (1 - wrap) + wrap
        p1, n1 = step_of(after, power_after)

        @pl.when((t < 2) | (t == 5))
        def _():
            settle(qq.at[0:pair, 0:HEAD], q_recv.at[p1])

        @pl.when((t == 1) | (t == 5) | (t == 9))
        def _():
            n2 = (t + 3) // 4
            pass_on(2 * n2)
            pass_on(2 * n2 + 1)

        @pl.when((t == 2) | (t == 7) | (t == 10))
        def _():
            receive(n1)

        for u in range(GROUP):
            use(p, n, u)
            fill(p1, n1, u)

        @pl.when((t > 10) & (t < 14))
        def _():
            for i in range(2):
                b = 2 * p + i
                obuf[query_rows(b), :] = result(b)
                out_copy(b).start()

        @pl.when(t == 15)
        def _():
            obuf[query_rows(1), :] = result(1)
            out_copy(1).start()
            att[:, cols(chip)] = result(0)

        return power_after

    lax.fori_loop(0, count, body, 1)
    for copy in loads:
        copy.wait()

    def core_copy(b):
        head = chip_at(b, 1)
        return remote(
            part_sib.at[head], part_in.at[head], sent.at[5], c_recv.at[b], chip, 1 - core
        )

    def share(group):
        heads = [chip_at(b, 1) for b in group]
        turned = jnp.concatenate([att[:, cols(head)].T for head in heads], axis=0)
        theirs = jnp.dot(turned, g_sib[...], preferred_element_type=jnp.float32).astype(jnp.bfloat16)
        for i, head in enumerate(heads):
            part_sib[head] = theirs[i * HEAD : (i + 1) * HEAD]
        for b in group:
            core_copy(b).start()
        ours = jnp.dot(turned, g_own[...], preferred_element_type=jnp.float32)
        for i, head in enumerate(heads):
            part_own[head] = ours[i * HEAD : (i + 1) * HEAD]

    def z_copy(head, d):
        return pltpu.make_async_remote_copy(
            src_ref=tiles[0][0].at[head // 4, head % 4], dst_ref=landed[0][0].at[d - 1, head // 4],
            send_sem=r_send.at[0, 0], recv_sem=r_recv.at[0, 0], device_id=peer("z", d), device_id_type=MESH,
        )

    def y_copy(head, d):
        return pltpu.make_async_remote_copy(
            src_ref=tiles[1][0].at[head, (row_y + d) % 4], dst_ref=landed[1][0].at[d - 1, head],
            send_sem=r_send.at[1, 0], recv_sem=r_recv.at[1, 0], device_id=peer("y", d), device_id_type=MESH,
        )

    def x_copy(hi, part, d):
        to = (x + d) % 4
        at = pl.ds(hi * 4, 4)
        return pltpu.make_async_remote_copy(
            src_ref=tiles[2][0].at[part, at, to // 2], dst_ref=landed[2][0].at[d - 1, at],
            send_sem=r_send.at[2, 0], recv_sem=r_recv.at[2, 0], device_id=peer("x", d), device_id_type=MESH,
        )

    def join_cores(b):
        core_copy(b).wait_recv()
        head = chip_at(b, 1)
        both = part_own[head] + part_in[head].astype(jnp.float32)
        a0, a1 = PARTS[0], PARTS[0] + PARTS[1]
        lo, hi = head // 4, head % 4
        tiles[0][0][lo, hi] = both[:, 0:a0].astype(jnp.bfloat16).reshape(8, 16, a0)
        tiles[1][0][head] = both[:, a0:a1].astype(jnp.bfloat16).reshape(4, 2, 16, a1 - a0)
        tiles[2][0][lo, pl.ds(hi * 4, 4)] = (
            both[:, a1:].astype(jnp.bfloat16).reshape(4, 2, 16, half - a1)
        )
        dz = (hi - z + 4) % 4

        @pl.when(dz > 0)
        def _():
            z_copy(head, dz).start()

        for d in (1, 3, 2):
            y_copy(head, d).start()
        for to_hi in range(2):
            dx = (to_hi * 2 + lo - x + 4) % 4

            @pl.when(dx > 0)
            def _():
                x_copy(hi, lo, dx).start()

    for i, group in enumerate(HOME):
        for b in group:
            if b:
                out_copy(b).wait_recv()
        share(group)
        if i:
            for b in HOME[i - 1]:
                join_cores(b)
    for b in HOME[-1]:
        join_cores(b)

    def block(part, stage, d):
        tile = tiles[part][stage]
        axis = ORDERS[part][stage]
        if axis == "x":
            to = (x + d) % 4
            if part == 0:
                return tile.at[to % 2, to // 2]
            return tile.at[to % 2, :, to // 2]
        to = ((z if axis == "z" else row_y) + d) % 4
        if (part, stage) in ((0, 0), (0, 1), (1, 0)):
            return tile.at[:, to]
        return tile.at[to]

    def block_copy(part, stage, d):
        return pltpu.make_async_remote_copy(
            src_ref=block(part, stage, d), dst_ref=landed[part][stage].at[d - 1],
            send_sem=r_send.at[part, stage], recv_sem=r_recv.at[part, stage],
            device_id=peer(ORDERS[part][stage], d), device_id_type=MESH,
        )

    def send(part, stage):
        for d in (1, 3, 2):
            block_copy(part, stage, d).start()

    def total(part, stage):
        settle(landed[part][stage], r_recv.at[part, stage])
        value = block(part, stage, 0)[...].astype(jnp.float32)
        for d in range(3):
            value = value + landed[part][stage][d].astype(jnp.float32)
        return value

    def mix(i, unused):
        at = pl.ds(pl.multiple_of(i * 512, 512), 512)
        mixed[:, at] = jnp.dot(att[...], w_buf[:, at], preferred_element_type=jnp.float32).astype(
            jnp.bfloat16
        )
        return unused

    for part in FIRST:
        tiles[part][1][...] = total(part, 0).astype(jnp.bfloat16).reshape(tiles[part][1].shape)
        send(part, 1)

    def last_copies(part):
        copies = []
        for d in (0, 1, 3, 2):
            for other in range(2):
                if d or other:
                    slot = 3 + d if other else d - 1
                    to = (core + other) % 2
                    target = dict(peer(ORDERS[part][2], d))
                    target["seq"] = target.get("seq", seq) + to - core
                    copies.append(
                        pltpu.make_async_remote_copy(
                            src_ref=block(part, 2, d).at[to], dst_ref=landed[part][2].at[slot],
                            send_sem=r_send.at[part, 2], recv_sem=r_recv.at[part, 2],
                            device_id=target, device_id_type=MESH,
                        )
                    )
        return copies

    lax.fori_loop(0, w_buf.shape[1] // 512, mix, 0)
    mixed_copy = pltpu.make_async_copy(mixed, mixed_ref, local_sem.at[7])
    mixed_copy.start()

    for part in FIRST:
        tiles[part][2][...] = total(part, 1).reshape(tiles[part][2].shape)
        for copy in last_copies(part):
            copy.start()
    for part in FIRST:
        at = sum(PARTS[:part])
        settle(landed[part][2], r_recv.at[part, 2])
        ours = block(part, 2, 0).at[core][...]
        for d in range(3):
            ours = ours + landed[part][2][d]
        theirs = landed[part][2][3]
        for d in range(4, 7):
            theirs = theirs + landed[part][2][d]
        grad[:, pl.ds(pl.multiple_of(core * half + at, HEAD), PARTS[part])] = ours
        grad[:, pl.ds(pl.multiple_of((1 - core) * half + at, HEAD), PARTS[part])] = theirs

    mixed_copy.wait()
    some = (CHIPS - 1) * rows
    settle(ends.at[0 : 2 * CHIPS - 1], sent.at[0])
    settle(qq.at[0:some, 0:HEAD], sent.at[1])
    settle(kk.at[0 : 2 * some, 0:HEAD], sent.at[2])
    settle(kk.at[:, 0:HEAD], sent.at[3])
    settle(obuf.at[0:some, :], sent.at[4])
    settle(part_sib, sent.at[5])
    for part in range(3):
        for stage in range(3):
            settle(landed[part][stage], r_send.at[part, stage])


def attend(q, k, v, ends, w, g):
    rows, width = q.shape
    out = w.shape[1]
    half = out // 2
    pair = 2 * rows
    tokens = CHIPS * pair
    mine = CHIPS * rows
    dma = pltpu.SemaphoreType.DMA
    bf16 = jnp.bfloat16
    p0, p1, p2 = PARTS
    tiles = (
        (
            pltpu.VMEM((2, 4, 8, 16, p0), bf16),
            pltpu.VMEM((2, 4, 2, 16, p0), bf16),
            pltpu.VMEM((2, 2, 2, 8, p0), jnp.float32),
        ),
        (
            pltpu.VMEM((8, 4, 2, 16, p1), bf16),
            pltpu.VMEM((2, 4, 2, 16, p1), bf16),
            pltpu.VMEM((4, 2, 8, p1), jnp.float32),
        ),
        (
            pltpu.VMEM((2, 16, 2, 16, p2), bf16),
            pltpu.VMEM((4, 4, 16, p2), bf16),
            pltpu.VMEM((4, 2, 8, p2), jnp.float32),
        ),
    )
    landed = (
        (
            pltpu.VMEM((3, 2, 8, 16, p0), bf16),
            pltpu.VMEM((3, 2, 2, 16, p0), bf16),
            pltpu.VMEM((7, 8, p0), jnp.float32),
        ),
        (
            pltpu.VMEM((3, 8, 2, 16, p1), bf16),
            pltpu.VMEM((3, 4, 16, p1), bf16),
            pltpu.VMEM((7, 8, p1), jnp.float32),
        ),
        (
            pltpu.VMEM((3, 16, 16, p2), bf16),
            pltpu.VMEM((3, 4, 16, p2), bf16),
            pltpu.VMEM((7, 8, p2), jnp.float32),
        ),
    )
    return pl.pallas_call(
        functools.partial(attend_kernel, rows),
        out_shape=(
            jax.ShapeDtypeStruct((rows, out), bf16),
            jax.ShapeDtypeStruct((8, out), jnp.float32),
        ),
        in_specs=[pl.BlockSpec(memory_space=pl.ANY)] * 6,
        out_specs=(pl.BlockSpec(memory_space=pl.ANY), pl.BlockSpec(memory_space=pltpu.VMEM)),
        scratch_shapes=[
            pltpu.VMEM((mine, 2 * HEAD), bf16),
            pltpu.VMEM((tokens, 2 * HEAD), bf16),
            pltpu.VMEM((tokens, HEAD), bf16),
            pltpu.VMEM((HEAD + ONES, tokens), bf16),
            pltpu.VMEM((2 * CHIPS, 1, rows), jnp.int32),
            pltpu.VMEM((HEAD + ONES, mine), jnp.float32),
            pltpu.VMEM((8, mine), jnp.float32),
            pltpu.VMEM((GROUP, 2 * pair, WIDE), jnp.float32),
            pltpu.VMEM((GROUP, 8, WIDE), jnp.float32),
            pltpu.VMEM((mine, HEAD), bf16),
            dma((8,)),
            dma((4,)), dma((CHIPS,)), dma((4,)), dma((CHIPS,)), dma((CHIPS,)), dma((1,)),
            dma((3, 3)), dma((3, 3)), dma((6,)),
            pltpu.VMEM((rows, width), bf16),
            pltpu.VMEM((width, out), bf16),
            pltpu.VMEM((rows, half), bf16),
            pltpu.VMEM((rows, half), bf16),
            pltpu.VMEM((rows, out), bf16),
            pltpu.VMEM((CHIPS, HEAD, half), jnp.float32),
            pltpu.VMEM((CHIPS, HEAD, half), bf16),
            pltpu.VMEM((CHIPS, HEAD, half), bf16),
            tiles,
            landed,
        ],
        compiler_params=pltpu.CompilerParams(
            collective_id=0, has_side_effects=True, vmem_limit_bytes=60 << 20
        ),
    )(q, k, v, ends, w, g)


def hand_over_kernel(mixed_ref, grad_ref, mixed_out_ref, grad_out_ref, mixed, grad, sem):
    rows = mixed.shape[0] // PIECES
    arrays = [(grad_ref, grad_out_ref, grad)]
    for i in range(PIECES):
        at = pl.ds(i * rows, rows)
        arrays.append((mixed_ref.at[at, :], mixed_out_ref.at[at, :], mixed.at[at, :]))
    into = [
        pltpu.make_async_copy(source, held, sem.at[0, i]) for i, (source, _, held) in enumerate(arrays)
    ]
    out = [
        pltpu.make_async_copy(held, target, sem.at[1, i]) for i, (_, target, held) in enumerate(arrays)
    ]
    for copy in into:
        copy.start()
    for i in range(len(arrays)):
        into[i].wait()
        out[i].start()
    for copy in out:
        copy.wait()


def hand_over(mixed, grad):
    any_space = pl.BlockSpec(memory_space=pl.ANY)
    return pl.pallas_call(
        hand_over_kernel,
        out_shape=(
            jax.ShapeDtypeStruct(mixed.shape, mixed.dtype),
            jax.ShapeDtypeStruct(grad.shape, grad.dtype),
        ),
        in_specs=[any_space] * 2,
        out_specs=(any_space,) * 2,
        scratch_shapes=[
            pltpu.VMEM(mixed.shape, mixed.dtype),
            pltpu.VMEM(grad.shape, grad.dtype),
            pltpu.SemaphoreType.DMA((2, PIECES + 1)),
        ],
        compiler_params=pltpu.CompilerParams(vmem_limit_bytes=60 << 20),
    )(mixed, grad)


def body(query_rows, key_rows, value_rows, scale_end, out_weight, grad_out):
    mixed_out, out_grad = hand_over(
        *attend(query_rows[0], key_rows[0], value_rows[0], scale_end, out_weight, grad_out[0])
    )
    return (mixed_out[None], out_grad)


def solution(mesh):
    torus = Mesh(mesh.devices.reshape(2, 4, mesh.shape["seq"]), ("dp_0", "dp_1", "seq"))
    in_specs = (
        P(DP, "seq", None),
        P(DP, "seq", None),
        P(DP, "seq", None),
        P("seq"),
        P(),
        P(DP, "seq", None),
    )
    out_specs = (P(DP, "seq", None), P(DP_SEQ, None))
    return jax.shard_map(body, mesh=torus, in_specs=in_specs, out_specs=out_specs, check_vma=False)
```

```python
import functools
import math

import jax
import jax.numpy as jnp
from jax import lax
from jax.experimental import pallas as pl
from jax.experimental.pallas import tpu as pltpu
from jax.sharding import Mesh
from jax.sharding import PartitionSpec as P

HEAD = 128
DP = ("dp_0", "dp_1")
PARTS = (256, 384, 384)
ORDERS = ("zyx", "yxz", "xzy")
FIRST = (2, 1, 0)
STEPS = (
    (0, 0), (1, 0), (3, 0), (2, 0), (0, 1), (1, 1), (3, 1), (2, 1),
    (3, 2), (2, 2), (1, 2), (0, 2), (3, 3), (2, 3), (1, 3), (0, 3),
)
HOME = ((0, 6), (7, 5), (4, 2), (3, 1))
DP_SEQ = ("dp_0", "dp_1", "seq")
MESH = pl.DeviceIdType.MESH
LOG2_SCALE = HEAD ** (-0.5) * math.log2(math.e)
LOW = -1e30
HIDE = -(2.0**100)
CHIPS = 8
PIECES = 4
WIDE = 256
GROUP = 3
ONES = 16


def digits(values, base):
    return sum(value * base**i for i, value in enumerate(values))


def attend_kernel(
    rows,
    q_ref, k_ref, v_ref, end_ref, w_ref, g_ref, mixed_ref, grad,
    qq, kk, vals, vt, ends, acc, top, sbuf, sbuf_top, obuf,
    local_sem, q_recv, kv_recv, f_recv, o_recv, c_recv, e_recv, r_send, r_recv, sent,
    att, w_buf, g_own, g_sib, mixed, part_own, part_sib, part_in, tiles, landed,
):
    seq = lax.axis_index("seq")
    x_lo = lax.axis_index("dp_0")
    z = lax.axis_index("dp_1")
    half = g_own.shape[1]
    chip = seq // 2
    core = seq % 2
    row_y = chip // 2
    col_x = chip % 2
    pair = 2 * rows
    tokens = CHIPS * pair
    step_rows = GROUP * WIDE
    step_keys = 2 * pair

    def chip_at(b, sign):
        late, i = b // 4, b % 4
        dx = (1 - late) * (i // 3) + late * (1 - i % 2 * (1 - i // 3))
        dy = (1 - late) * (i % 3 + i % 3 // 2) + late * (i + 1 - 2 * (i // 3))
        return ((row_y + sign * dy + 4) % 4) * 2 + (col_x + dx) % 2

    barrier = pltpu.get_barrier_semaphore()
    for i in range(1, 2 * CHIPS):
        pl.semaphore_signal(
            barrier, inc=1, device_id={"seq": (seq + i) % (2 * CHIPS)}, device_id_type=MESH
        )
    x = col_x * 2 + x_lo

    def peer(axis, d):
        if axis == "z":
            return {"dp_1": (z + d) % 4}
        if axis == "y":
            return {"seq": ((row_y + d) % 4) * 4 + col_x * 2 + core}
        to = (x + d) % 4
        return {"dp_0": to % 2, "seq": row_y * 4 + (to // 2) * 2 + core}

    for axis, d in (("x", 1), ("x", 3), ("z", 1), ("z", 2), ("z", 3)):
        pl.semaphore_signal(barrier, inc=1, device_id=peer(axis, d), device_id_type=MESH)
    pl.semaphore_wait(barrier, 2 * CHIPS + 4)

    def cols(head):
        return pl.ds(pl.multiple_of(head * HEAD, HEAD), HEAD)

    def token_rows(b, j):
        return pl.ds(pl.multiple_of((b * 2 + j) * rows, rows), rows)

    def query_rows(b):
        return pl.ds(pl.multiple_of(b * rows, rows), rows)

    def remote(src, dst, send, recv, c, j):
        return pltpu.make_async_remote_copy(
            src_ref=src, dst_ref=dst, send_sem=send, recv_sem=recv,
            device_id={"seq": c * 2 + j}, device_id_type=MESH,
        )

    def settle(array, sem):
        pltpu.make_async_copy(array, array, sem).wait()

    def end_copy(to):
        return pltpu.make_async_remote_copy(
            src_ref=end_ref, dst_ref=ends.at[seq, 0], send_sem=sent.at[0], recv_sem=e_recv.at[0],
            device_id={"seq": to}, device_id_type=MESH,
        )

    def send_queries(b):
        to = chip_at(b, 1)
        remote(
            q_ref.at[:, cols(to)], qq.at[query_rows(b), 0:HEAD], sent.at[1], q_recv.at[b // 2], to, core
        ).start()

    def send_keys(b):
        to = chip_at(b, 1)
        at = token_rows(b, core)
        remote(
            k_ref.at[:, cols(to)], kk.at[at, 0:HEAD], sent.at[2], kv_recv.at[b], to, core
        ).start()
        remote(v_ref.at[:, cols(to)], vals.at[at, :], sent.at[2], kv_recv.at[b], to, core).start()

    def forward(b):
        at = token_rows(b, core)
        remote(
            kk.at[at, 0:HEAD], kk.at[at, 0:HEAD], sent.at[3], f_recv.at[b // 2], chip, 1 - core
        ).start()
        remote(
            vals.at[at, :], vals.at[at, :], sent.at[3], f_recv.at[b // 2], chip, 1 - core
        ).start()

    own = [
        pltpu.make_async_copy(
            k_ref.at[:, cols(chip)], kk.at[token_rows(0, core), 0:HEAD], local_sem.at[0]
        ),
        pltpu.make_async_copy(
            v_ref.at[:, cols(chip)], vals.at[token_rows(0, core), :], local_sem.at[1]
        ),
        pltpu.make_async_copy(
            q_ref.at[:, cols(chip)], qq.at[query_rows(0), 0:HEAD], local_sem.at[2]
        ),
        pltpu.make_async_copy(end_ref, ends.at[seq, 0], local_sem.at[3]),
    ]
    for i in range(1, 2 * CHIPS):
        end_copy((seq + i) % (2 * CHIPS)).start()
    for copy in own:
        copy.start()
    for b in (1, 2):
        send_keys(b)
        send_queries(b)
    for b in (3, 4, 6, 7, 5):
        send_queries(b)
    own[0].wait()
    own[1].wait()
    forward(0)

    loads = [
        pltpu.make_async_copy(g_ref.at[:, pl.ds(pl.multiple_of(core * half, half), half)], g_own, local_sem.at[4]),
        pltpu.make_async_copy(
            g_ref.at[:, pl.ds(pl.multiple_of((1 - core) * half, half), half)], g_sib, local_sem.at[5]
        ),
        pltpu.make_async_copy(w_ref, w_buf, local_sem.at[6]),
    ]
    for copy in loads:
        copy.start()
    vt[HEAD:, :] = jnp.ones((ONES, tokens), jnp.bfloat16)
    acc[...] = jnp.zeros_like(acc)
    top[...] = jnp.full_like(top, LOW)
    own[2].wait()
    own[3].wait()
    settle(ends.at[0 : 2 * CHIPS - 1], e_recv.at[0])

    every = ends[...].astype(jnp.float32)

    def least(x):
        return jnp.min(jnp.min(x, axis=0), axis=1, keepdims=True)

    whole = jnp.float32(tokens)
    first = least(every)
    second = least(jnp.where(every > first, every, whole))
    third = least(jnp.where(every > second, every, whole))
    lane = lax.broadcasted_iota(jnp.int32, (1, HEAD), 1)
    stop = jnp.where(lane == 0, first, jnp.where(lane == 1, second, jnp.where(lane == 2, third, whole)))
    start = jnp.where(
        lane == 0, jnp.float32(0), jnp.where(lane == 1, first, jnp.where(lane == 2, second, third))
    )
    start = jnp.where(lane < 4, start, 2.0 * whole)

    def hide_keys(b, unused):
        base = chip_at(b, -1) * pair
        at = (base + lax.broadcasted_iota(jnp.int32, (pair, HEAD), 0)).astype(jnp.float32)
        kk[pl.ds(pl.multiple_of(b * pair, pair), pair), HEAD:] = jnp.where(
            at >= stop, HIDE, 0.0
        ).astype(jnp.bfloat16)
        return unused

    lax.fori_loop(0, CHIPS, hide_keys, 0)

    def mark_queries(b, unused):
        base = (chip_at(b, -1) * 2 + core) * rows
        at = (base + lax.broadcasted_iota(jnp.int32, (rows, HEAD), 0)).astype(jnp.float32)
        inside = jnp.where(at >= start, 1.0, 0.0) * jnp.where(at < stop, 1.0, 0.0)
        qq[query_rows(b), HEAD:] = inside.astype(jnp.bfloat16)
        return unused

    lax.fori_loop(0, CHIPS, mark_queries, 0)

    for b in range(3, CHIPS):
        send_keys(b)

    half_steps = len(STEPS) // 2

    def step_of(t, power):
        late = t // half_steps
        first = [digits([step[i] for step in STEPS[:half_steps]], 4) for i in range(2)]
        second = [digits([step[i] for step in STEPS[half_steps:]], 4) for i in range(2)]
        return [(a + late * (b - a)) // power % 4 for a, b in zip(first, second)]

    def key_rows(n):
        return pl.ds(pl.multiple_of(n * step_keys, step_keys), step_keys)

    def pass_on(b):
        settle(kk.at[0:pair, 0:HEAD], kv_recv.at[b])
        forward(b)

    def receive(n):
        settle(kk.at[0:step_keys, 0:HEAD], f_recv.at[n])
        at = key_rows(n)
        vt[0:HEAD, at] = vals[at, :].T

    def fill(p, n, u):
        queries = pl.ds(pl.multiple_of(p * step_rows + u * WIDE, WIDE), WIDE)
        scores = lax.dot_general(
            kk[key_rows(n), :], qq[queries, :], (((1,), (1,)), ((), ())),
            preferred_element_type=jnp.float32,
        )
        sbuf_top[u, 0:1, :] = jnp.max(scores, axis=0, keepdims=True)
        sbuf[u] = scores

    def use(p, n, u):
        queries = pl.ds(pl.multiple_of(p * step_rows + u * WIDE, WIDE), WIDE)
        old = top[0:1, queries]
        new = jnp.maximum(old, sbuf_top[u, 0:1, :])
        top[0:1, queries] = new
        weights = jnp.exp2(sbuf[u] * LOG2_SCALE - new * LOG2_SCALE).astype(jnp.bfloat16)
        factor = jnp.exp2((old - new) * LOG2_SCALE)
        product = jnp.dot(vt[:, key_rows(n)], weights, preferred_element_type=jnp.float32)
        acc[:, queries] = acc[:, queries] * factor + product

    def out_copy(b):
        return remote(
            obuf.at[query_rows(b), :], att.at[:, cols(chip)], sent.at[4], o_recv.at[b],
            chip_at(b, -1), core,
        )

    def result(b):
        at = query_rows(b)
        return (acc[0:HEAD, at] / acc[HEAD : HEAD + 1, at]).T.astype(jnp.bfloat16)

    settle(qq.at[0:rows, 0:HEAD], q_recv.at[0])
    pass_on(1)
    receive(0)
    for u in range(GROUP):
        fill(0, 0, u)
    count = len(STEPS)

    def body(t, power):
        p, n = step_of(t, power)
        after = jnp.minimum(t + 1, count - 1)
        wrap = t % half_steps // (half_steps - 1)
        power_after = power * 4 * (1 - wrap) + wrap
        p1, n1 = step_of(after, power_after)

        @pl.when(t < 3)
        def _():
            settle(qq.at[0:pair, 0:HEAD], q_recv.at[p1])

        @pl.when((t == 2) | (t == 6) | (t == 10))
        def _():
            n2 = t // 4 + 1
            pass_on(2 * n2)
            pass_on(2 * n2 + 1)

        @pl.when((t == 3) | (t == 7) | (t == 11))
        def _():
            receive(n1)

        for u in range(GROUP):
            use(p, n, u)
            fill(p1, n1, u)

        @pl.when((t > 11) & (t < 15))
        def _():
            for i in range(2):
                b = 2 * p + i
                obuf[query_rows(b), :] = result(b)
                out_copy(b).start()

        @pl.when(t == 15)
        def _():
            obuf[query_rows(1), :] = result(1)
            out_copy(1).start()
            att[:, cols(chip)] = result(0)

        return power_after

    lax.fori_loop(0, count, body, 1)
    for copy in loads:
        copy.wait()

    def core_copy(b):
        head = chip_at(b, 1)
        return remote(
            part_sib.at[head], part_in.at[head], sent.at[5], c_recv.at[b], chip, 1 - core
        )

    def share(group):
        heads = [chip_at(b, 1) for b in group]
        turned = jnp.concatenate([att[:, cols(head)].T for head in heads], axis=0)
        theirs = jnp.dot(turned, g_sib[...], preferred_element_type=jnp.float32).astype(jnp.bfloat16)
        for i, head in enumerate(heads):
            part_sib[head] = theirs[i * HEAD : (i + 1) * HEAD]
        for b in group:
            core_copy(b).start()
        ours = jnp.dot(turned, g_own[...], preferred_element_type=jnp.float32)
        for i, head in enumerate(heads):
            part_own[head] = ours[i * HEAD : (i + 1) * HEAD]

    def z_copy(head, d):
        return pltpu.make_async_remote_copy(
            src_ref=tiles[0][0].at[head // 4, head % 4], dst_ref=landed[0][0].at[d - 1, head // 4],
            send_sem=r_send.at[0, 0], recv_sem=r_recv.at[0, 0], device_id=peer("z", d), device_id_type=MESH,
        )

    def y_copy(head, d):
        return pltpu.make_async_remote_copy(
            src_ref=tiles[1][0].at[head, (row_y + d) % 4], dst_ref=landed[1][0].at[d - 1, head],
            send_sem=r_send.at[1, 0], recv_sem=r_recv.at[1, 0], device_id=peer("y", d), device_id_type=MESH,
        )

    def x_copy(hi, part, d):
        to = (x + d) % 4
        at = pl.ds(hi * 4, 4)
        return pltpu.make_async_remote_copy(
            src_ref=tiles[2][0].at[part, at, to // 2], dst_ref=landed[2][0].at[d - 1, at],
            send_sem=r_send.at[2, 0], recv_sem=r_recv.at[2, 0], device_id=peer("x", d), device_id_type=MESH,
        )

    def join_cores(b):
        core_copy(b).wait_recv()
        head = chip_at(b, 1)
        both = part_own[head] + part_in[head].astype(jnp.float32)
        a0, a1 = PARTS[0], PARTS[0] + PARTS[1]
        lo, hi = head // 4, head % 4
        tiles[0][0][lo, hi] = both[:, 0:a0].astype(jnp.bfloat16).reshape(8, 16, a0)
        tiles[1][0][head] = both[:, a0:a1].astype(jnp.bfloat16).reshape(4, 2, 16, a1 - a0)
        tiles[2][0][lo, pl.ds(hi * 4, 4)] = (
            both[:, a1:].astype(jnp.bfloat16).reshape(4, 2, 16, half - a1)
        )
        dz = (hi - z + 4) % 4

        @pl.when(dz > 0)
        def _():
            z_copy(head, dz).start()

        for d in (1, 3, 2):
            y_copy(head, d).start()
        for to_hi in range(2):
            dx = (to_hi * 2 + lo - x + 4) % 4

            @pl.when(dx > 0)
            def _():
                x_copy(hi, lo, dx).start()

    for i, group in enumerate(HOME):
        for b in group:
            if b:
                out_copy(b).wait_recv()
        share(group)
        if i:
            for b in HOME[i - 1]:
                join_cores(b)
    for b in HOME[-1]:
        join_cores(b)

    def block(part, stage, d):
        tile = tiles[part][stage]
        axis = ORDERS[part][stage]
        if axis == "x":
            to = (x + d) % 4
            if part == 0:
                return tile.at[to % 2, to // 2]
            return tile.at[to % 2, :, to // 2]
        to = ((z if axis == "z" else row_y) + d) % 4
        if (part, stage) in ((0, 0), (0, 1), (1, 0)):
            return tile.at[:, to]
        return tile.at[to]

    def block_copy(part, stage, d):
        return pltpu.make_async_remote_copy(
            src_ref=block(part, stage, d), dst_ref=landed[part][stage].at[d - 1],
            send_sem=r_send.at[part, stage], recv_sem=r_recv.at[part, stage],
            device_id=peer(ORDERS[part][stage], d), device_id_type=MESH,
        )

    def send(part, stage):
        for d in (1, 3, 2):
            block_copy(part, stage, d).start()

    def total(part, stage):
        settle(landed[part][stage], r_recv.at[part, stage])
        value = block(part, stage, 0)[...].astype(jnp.float32)
        for d in range(3):
            value = value + landed[part][stage][d].astype(jnp.float32)
        return value

    def mix(i, unused):
        at = pl.ds(pl.multiple_of(i * 512, 512), 512)
        mixed[:, at] = jnp.dot(att[...], w_buf[:, at], preferred_element_type=jnp.float32).astype(
            jnp.bfloat16
        )
        return unused

    lax.fori_loop(0, w_buf.shape[1] // 512, mix, 0)
    mixed_copy = pltpu.make_async_copy(mixed, mixed_ref, local_sem.at[7])
    mixed_copy.start()

    for part in FIRST:
        tiles[part][1][...] = total(part, 0).astype(jnp.bfloat16).reshape(tiles[part][1].shape)
        send(part, 1)

    def last_copies(part):
        copies = []
        for d in (0, 1, 3, 2):
            for other in range(2):
                if d or other:
                    slot = 3 + d if other else d - 1
                    to = (core + other) % 2
                    target = dict(peer(ORDERS[part][2], d))
                    target["seq"] = target.get("seq", seq) + to - core
                    copies.append(
                        pltpu.make_async_remote_copy(
                            src_ref=block(part, 2, d).at[to], dst_ref=landed[part][2].at[slot],
                            send_sem=r_send.at[part, 2], recv_sem=r_recv.at[part, 2],
                            device_id=target, device_id_type=MESH,
                        )
                    )
        return copies

    for part in FIRST:
        tiles[part][2][...] = total(part, 1).reshape(tiles[part][2].shape)
        for copy in last_copies(part):
            copy.start()
    for part in FIRST:
        at = sum(PARTS[:part])
        settle(landed[part][2], r_recv.at[part, 2])
        ours = block(part, 2, 0).at[core][...]
        for d in range(3):
            ours = ours + landed[part][2][d]
        theirs = landed[part][2][3]
        for d in range(4, 7):
            theirs = theirs + landed[part][2][d]
        grad[:, pl.ds(pl.multiple_of(core * half + at, HEAD), PARTS[part])] = ours
        grad[:, pl.ds(pl.multiple_of((1 - core) * half + at, HEAD), PARTS[part])] = theirs

    mixed_copy.wait()
    some = (CHIPS - 1) * rows
    settle(ends.at[0 : 2 * CHIPS - 1], sent.at[0])
    settle(qq.at[0:some, 0:HEAD], sent.at[1])
    settle(kk.at[0 : 2 * some, 0:HEAD], sent.at[2])
    settle(kk.at[:, 0:HEAD], sent.at[3])
    settle(obuf.at[0:some, :], sent.at[4])
    settle(part_sib, sent.at[5])
    for part in range(3):
        for stage in range(3):
            settle(landed[part][stage], r_send.at[part, stage])


def attend(q, k, v, ends, w, g):
    rows, width = q.shape
    out = w.shape[1]
    half = out // 2
    pair = 2 * rows
    tokens = CHIPS * pair
    mine = CHIPS * rows
    dma = pltpu.SemaphoreType.DMA
    bf16 = jnp.bfloat16
    p0, p1, p2 = PARTS
    tiles = (
        (
            pltpu.VMEM((2, 4, 8, 16, p0), bf16),
            pltpu.VMEM((2, 4, 2, 16, p0), bf16),
            pltpu.VMEM((2, 2, 2, 8, p0), jnp.float32),
        ),
        (
            pltpu.VMEM((8, 4, 2, 16, p1), bf16),
            pltpu.VMEM((2, 4, 2, 16, p1), bf16),
            pltpu.VMEM((4, 2, 8, p1), jnp.float32),
        ),
        (
            pltpu.VMEM((2, 16, 2, 16, p2), bf16),
            pltpu.VMEM((4, 4, 16, p2), bf16),
            pltpu.VMEM((4, 2, 8, p2), jnp.float32),
        ),
    )
    landed = (
        (
            pltpu.VMEM((3, 2, 8, 16, p0), bf16),
            pltpu.VMEM((3, 2, 2, 16, p0), bf16),
            pltpu.VMEM((7, 8, p0), jnp.float32),
        ),
        (
            pltpu.VMEM((3, 8, 2, 16, p1), bf16),
            pltpu.VMEM((3, 4, 16, p1), bf16),
            pltpu.VMEM((7, 8, p1), jnp.float32),
        ),
        (
            pltpu.VMEM((3, 16, 16, p2), bf16),
            pltpu.VMEM((3, 4, 16, p2), bf16),
            pltpu.VMEM((7, 8, p2), jnp.float32),
        ),
    )
    return pl.pallas_call(
        functools.partial(attend_kernel, rows),
        out_shape=(
            jax.ShapeDtypeStruct((rows, out), bf16),
            jax.ShapeDtypeStruct((8, out), jnp.float32),
        ),
        in_specs=[pl.BlockSpec(memory_space=pl.ANY)] * 6,
        out_specs=(pl.BlockSpec(memory_space=pl.ANY), pl.BlockSpec(memory_space=pltpu.VMEM)),
        scratch_shapes=[
            pltpu.VMEM((mine, 2 * HEAD), bf16),
            pltpu.VMEM((tokens, 2 * HEAD), bf16),
            pltpu.VMEM((tokens, HEAD), bf16),
            pltpu.VMEM((HEAD + ONES, tokens), bf16),
            pltpu.VMEM((2 * CHIPS, 1, rows), jnp.int32),
            pltpu.VMEM((HEAD + ONES, mine), jnp.float32),
            pltpu.VMEM((8, mine), jnp.float32),
            pltpu.VMEM((GROUP, 2 * pair, WIDE), jnp.float32),
            pltpu.VMEM((GROUP, 8, WIDE), jnp.float32),
            pltpu.VMEM((mine, HEAD), bf16),
            dma((8,)),
            dma((4,)), dma((CHIPS,)), dma((4,)), dma((CHIPS,)), dma((CHIPS,)), dma((1,)),
            dma((3, 3)), dma((3, 3)), dma((6,)),
            pltpu.VMEM((rows, width), bf16),
            pltpu.VMEM((width, out), bf16),
            pltpu.VMEM((rows, half), bf16),
            pltpu.VMEM((rows, half), bf16),
            pltpu.VMEM((rows, out), bf16),
            pltpu.VMEM((CHIPS, HEAD, half), jnp.float32),
            pltpu.VMEM((CHIPS, HEAD, half), bf16),
            pltpu.VMEM((CHIPS, HEAD, half), bf16),
            tiles,
            landed,
        ],
        compiler_params=pltpu.CompilerParams(
            collective_id=0, has_side_effects=True, vmem_limit_bytes=60 << 20
        ),
    )(q, k, v, ends, w, g)


def hand_over_kernel(mixed_ref, grad_ref, mixed_out_ref, grad_out_ref, mixed, grad, sem):
    rows = mixed.shape[0] // PIECES
    arrays = [(grad_ref, grad_out_ref, grad)]
    for i in range(PIECES):
        at = pl.ds(i * rows, rows)
        arrays.append((mixed_ref.at[at, :], mixed_out_ref.at[at, :], mixed.at[at, :]))
    into = [
        pltpu.make_async_copy(source, held, sem.at[0, i]) for i, (source, _, held) in enumerate(arrays)
    ]
    out = [
        pltpu.make_async_copy(held, target, sem.at[1, i]) for i, (_, target, held) in enumerate(arrays)
    ]
    for copy in into:
        copy.start()
    for i in range(len(arrays)):
        into[i].wait()
        out[i].start()
    for copy in out:
        copy.wait()


def hand_over(mixed, grad):
    any_space = pl.BlockSpec(memory_space=pl.ANY)
    return pl.pallas_call(
        hand_over_kernel,
        out_shape=(
            jax.ShapeDtypeStruct(mixed.shape, mixed.dtype),
            jax.ShapeDtypeStruct(grad.shape, grad.dtype),
        ),
        in_specs=[any_space] * 2,
        out_specs=(any_space,) * 2,
        scratch_shapes=[
            pltpu.VMEM(mixed.shape, mixed.dtype),
            pltpu.VMEM(grad.shape, grad.dtype),
            pltpu.SemaphoreType.DMA((2, PIECES + 1)),
        ],
        compiler_params=pltpu.CompilerParams(vmem_limit_bytes=60 << 20),
    )(mixed, grad)


def body(query_rows, key_rows, value_rows, scale_end, out_weight, grad_out):
    mixed_out, out_grad = hand_over(
        *attend(query_rows[0], key_rows[0], value_rows[0], scale_end, out_weight, grad_out[0])
    )
    return (mixed_out[None], out_grad)


def solution(mesh):
    torus = Mesh(mesh.devices.reshape(2, 4, mesh.shape["seq"]), ("dp_0", "dp_1", "seq"))
    in_specs = (
        P(DP, "seq", None),
        P(DP, "seq", None),
        P(DP, "seq", None),
        P("seq"),
        P(),
        P(DP, "seq", None),
    )
    out_specs = (P(DP, "seq", None), P(DP_SEQ, None))
    return jax.shard_map(body, mesh=torus, in_specs=in_specs, out_specs=out_specs, check_vma=False)
```

```python
import functools
import math

import jax
import jax.numpy as jnp
from jax import lax
from jax.experimental import pallas as pl
from jax.experimental.pallas import tpu as pltpu
from jax.sharding import Mesh
from jax.sharding import PartitionSpec as P

HEAD = 128
DP = ("dp_0", "dp_1")
PARTS = (256, 384, 384)
ORDERS = ("zyx", "yxz", "xzy")
FIRST = (2, 1, 0)
STEPS = (
    (0, 0), (1, 0), (3, 0), (2, 0), (0, 1), (1, 1), (3, 1), (2, 1),
    (3, 2), (2, 2), (1, 2), (0, 2), (3, 3), (2, 3), (1, 3), (0, 3),
)
HOME = ((0, 6), (4, 7), (2, 5), (1, 3))
DP_SEQ = ("dp_0", "dp_1", "seq")
MESH = pl.DeviceIdType.MESH
LOG2_SCALE = HEAD ** (-0.5) * math.log2(math.e)
LOW = -1e30
HIDE = -(2.0**100)
CHIPS = 8
PIECES = 4
WIDE = 256
GROUP = 3
ONES = 16


def digits(values, base):
    return sum(value * base**i for i, value in enumerate(values))


def attend_kernel(
    rows,
    q_ref, k_ref, v_ref, end_ref, w_ref, g_ref, mixed_ref, grad,
    qq, kk, vals, vt, ends, acc, top, sbuf, sbuf_top, obuf,
    local_sem, q_recv, kv_recv, f_recv, o_recv, c_recv, e_recv, r_send, r_recv, sent,
    att, w_buf, g_own, g_sib, mixed, part_own, part_sib, part_in, tiles, landed,
):
    seq = lax.axis_index("seq")
    x_lo = lax.axis_index("dp_0")
    z = lax.axis_index("dp_1")
    half = g_own.shape[1]
    chip = seq // 2
    core = seq % 2
    row_y = chip // 2
    col_x = chip % 2
    pair = 2 * rows
    tokens = CHIPS * pair
    step_rows = GROUP * WIDE
    step_keys = 2 * pair

    def chip_at(b, sign):
        late, i = b // 4, b % 4
        dx = (1 - late) * (i // 3) + late * (1 - i % 2 * (1 - i // 3))
        dy = (1 - late) * (i % 3 + i % 3 // 2) + late * (i + 1 - 2 * (i // 3))
        return ((row_y + sign * dy + 4) % 4) * 2 + (col_x + dx) % 2

    barrier = pltpu.get_barrier_semaphore()
    for i in range(1, 2 * CHIPS):
        pl.semaphore_signal(
            barrier, inc=1, device_id={"seq": (seq + i) % (2 * CHIPS)}, device_id_type=MESH
        )
    x = col_x * 2 + x_lo

    def peer(axis, d):
        if axis == "z":
            return {"dp_1": (z + d) % 4}
        if axis == "y":
            return {"seq": ((row_y + d) % 4) * 4 + col_x * 2 + core}
        to = (x + d) % 4
        return {"dp_0": to % 2, "seq": row_y * 4 + (to // 2) * 2 + core}

    for axis, d in (("x", 1), ("x", 3), ("z", 1), ("z", 2), ("z", 3)):
        pl.semaphore_signal(barrier, inc=1, device_id=peer(axis, d), device_id_type=MESH)
    pl.semaphore_wait(barrier, 2 * CHIPS + 4)

    def cols(head):
        return pl.ds(pl.multiple_of(head * HEAD, HEAD), HEAD)

    def token_rows(b, j):
        return pl.ds(pl.multiple_of((b * 2 + j) * rows, rows), rows)

    def query_rows(b):
        return pl.ds(pl.multiple_of(b * rows, rows), rows)

    def remote(src, dst, send, recv, c, j):
        return pltpu.make_async_remote_copy(
            src_ref=src, dst_ref=dst, send_sem=send, recv_sem=recv,
            device_id={"seq": c * 2 + j}, device_id_type=MESH,
        )

    def settle(array, sem):
        pltpu.make_async_copy(array, array, sem).wait()

    def end_copy(to):
        return pltpu.make_async_remote_copy(
            src_ref=end_ref, dst_ref=ends.at[seq, 0], send_sem=sent.at[0], recv_sem=e_recv.at[0],
            device_id={"seq": to}, device_id_type=MESH,
        )

    def send_queries(b):
        to = chip_at(b, 1)
        remote(
            q_ref.at[:, cols(to)], qq.at[query_rows(b), 0:HEAD], sent.at[1], q_recv.at[b // 2], to, core
        ).start()

    def send_keys(b):
        to = chip_at(b, 1)
        at = token_rows(b, core)
        remote(
            k_ref.at[:, cols(to)], kk.at[at, 0:HEAD], sent.at[2], kv_recv.at[b], to, core
        ).start()
        remote(v_ref.at[:, cols(to)], vals.at[at, :], sent.at[2], kv_recv.at[b], to, core).start()

    def forward(b):
        at = token_rows(b, core)
        remote(
            kk.at[at, 0:HEAD], kk.at[at, 0:HEAD], sent.at[3], f_recv.at[b // 2], chip, 1 - core
        ).start()
        remote(
            vals.at[at, :], vals.at[at, :], sent.at[3], f_recv.at[b // 2], chip, 1 - core
        ).start()

    own = [
        pltpu.make_async_copy(
            k_ref.at[:, cols(chip)], kk.at[token_rows(0, core), 0:HEAD], local_sem.at[0]
        ),
        pltpu.make_async_copy(
            v_ref.at[:, cols(chip)], vals.at[token_rows(0, core), :], local_sem.at[1]
        ),
        pltpu.make_async_copy(
            q_ref.at[:, cols(chip)], qq.at[query_rows(0), 0:HEAD], local_sem.at[2]
        ),
        pltpu.make_async_copy(end_ref, ends.at[seq, 0], local_sem.at[3]),
    ]
    for i in range(1, 2 * CHIPS):
        end_copy((seq + i) % (2 * CHIPS)).start()
    for copy in own:
        copy.start()
    for b in (1, 2):
        send_keys(b)
        send_queries(b)
    for b in (3, 4, 6, 7, 5):
        send_queries(b)
    own[0].wait()
    own[1].wait()
    forward(0)

    loads = [
        pltpu.make_async_copy(g_ref.at[:, pl.ds(pl.multiple_of(core * half, half), half)], g_own, local_sem.at[4]),
        pltpu.make_async_copy(
            g_ref.at[:, pl.ds(pl.multiple_of((1 - core) * half, half), half)], g_sib, local_sem.at[5]
        ),
        pltpu.make_async_copy(w_ref, w_buf, local_sem.at[6]),
    ]
    for copy in loads:
        copy.start()
    vt[HEAD:, :] = jnp.ones((ONES, tokens), jnp.bfloat16)
    acc[...] = jnp.zeros_like(acc)
    top[...] = jnp.full_like(top, LOW)
    own[2].wait()
    own[3].wait()
    settle(ends.at[0 : 2 * CHIPS - 1], e_recv.at[0])

    every = ends[...].astype(jnp.float32)

    def least(x):
        return jnp.min(jnp.min(x, axis=0), axis=1, keepdims=True)

    whole = jnp.float32(tokens)
    first = least(every)
    second = least(jnp.where(every > first, every, whole))
    third = least(jnp.where(every > second, every, whole))
    lane = lax.broadcasted_iota(jnp.int32, (1, HEAD), 1)
    stop = jnp.where(lane == 0, first, jnp.where(lane == 1, second, jnp.where(lane == 2, third, whole)))
    start = jnp.where(
        lane == 0, jnp.float32(0), jnp.where(lane == 1, first, jnp.where(lane == 2, second, third))
    )
    start = jnp.where(lane < 4, start, 2.0 * whole)

    def hide_keys(b, unused):
        base = chip_at(b, -1) * pair
        at = (base + lax.broadcasted_iota(jnp.int32, (pair, HEAD), 0)).astype(jnp.float32)
        kk[pl.ds(pl.multiple_of(b * pair, pair), pair), HEAD:] = jnp.where(
            at >= stop, HIDE, 0.0
        ).astype(jnp.bfloat16)
        return unused

    lax.fori_loop(0, CHIPS, hide_keys, 0)

    def mark_queries(b, unused):
        base = (chip_at(b, -1) * 2 + core) * rows
        at = (base + lax.broadcasted_iota(jnp.int32, (rows, HEAD), 0)).astype(jnp.float32)
        inside = jnp.where(at >= start, 1.0, 0.0) * jnp.where(at < stop, 1.0, 0.0)
        qq[query_rows(b), HEAD:] = inside.astype(jnp.bfloat16)
        return unused

    lax.fori_loop(0, CHIPS, mark_queries, 0)

    for b in range(3, CHIPS):
        send_keys(b)

    half_steps = len(STEPS) // 2

    def step_of(t, power):
        late = t // half_steps
        first = [digits([step[i] for step in STEPS[:half_steps]], 4) for i in range(2)]
        second = [digits([step[i] for step in STEPS[half_steps:]], 4) for i in range(2)]
        return [(a + late * (b - a)) // power % 4 for a, b in zip(first, second)]

    def key_rows(n):
        return pl.ds(pl.multiple_of(n * step_keys, step_keys), step_keys)

    def pass_on(b):
        settle(kk.at[0:pair, 0:HEAD], kv_recv.at[b])
        forward(b)

    def receive(n):
        settle(kk.at[0:step_keys, 0:HEAD], f_recv.at[n])
        at = key_rows(n)
        vt[0:HEAD, at] = vals[at, :].T

    def fill(p, n, u):
        queries = pl.ds(pl.multiple_of(p * step_rows + u * WIDE, WIDE), WIDE)
        scores = lax.dot_general(
            kk[key_rows(n), :], qq[queries, :], (((1,), (1,)), ((), ())),
            preferred_element_type=jnp.float32,
        )
        sbuf_top[u, 0:1, :] = jnp.max(scores, axis=0, keepdims=True)
        sbuf[u] = scores

    def use(p, n, u):
        queries = pl.ds(pl.multiple_of(p * step_rows + u * WIDE, WIDE), WIDE)
        old = top[0:1, queries]
        new = jnp.maximum(old, sbuf_top[u, 0:1, :])
        top[0:1, queries] = new
        weights = jnp.exp2(sbuf[u] * LOG2_SCALE - new * LOG2_SCALE).astype(jnp.bfloat16)
        factor = jnp.exp2((old - new) * LOG2_SCALE)
        product = jnp.dot(vt[:, key_rows(n)], weights, preferred_element_type=jnp.float32)
        acc[:, queries] = acc[:, queries] * factor + product

    def out_copy(b):
        return remote(
            obuf.at[query_rows(b), :], att.at[:, cols(chip)], sent.at[4], o_recv.at[b],
            chip_at(b, -1), core,
        )

    def result(b):
        at = query_rows(b)
        return (acc[0:HEAD, at] / acc[HEAD : HEAD + 1, at]).T.astype(jnp.bfloat16)

    settle(qq.at[0:rows, 0:HEAD], q_recv.at[0])
    pass_on(1)
    receive(0)
    for u in range(GROUP):
        fill(0, 0, u)
    count = len(STEPS)

    def body(t, power):
        p, n = step_of(t, power)
        after = jnp.minimum(t + 1, count - 1)
        wrap = t % half_steps // (half_steps - 1)
        power_after = power * 4 * (1 - wrap) + wrap
        p1, n1 = step_of(after, power_after)

        @pl.when(t < 3)
        def _():
            settle(qq.at[0:pair, 0:HEAD], q_recv.at[p1])

        @pl.when((t == 2) | (t == 6) | (t == 10))
        def _():
            n2 = t // 4 + 1
            pass_on(2 * n2)
            pass_on(2 * n2 + 1)

        @pl.when((t == 3) | (t == 7) | (t == 11))
        def _():
            receive(n1)

        for u in range(GROUP):
            use(p, n, u)
            fill(p1, n1, u)

        @pl.when((t > 11) & (t < 15))
        def _():
            for i in range(2):
                b = 2 * p + i
                obuf[query_rows(b), :] = result(b)
                out_copy(b).start()

        @pl.when(t == 15)
        def _():
            obuf[query_rows(1), :] = result(1)
            out_copy(1).start()
            att[:, cols(chip)] = result(0)

        return power_after

    lax.fori_loop(0, count, body, 1)
    for copy in loads:
        copy.wait()

    def core_copy(b):
        head = chip_at(b, 1)
        return remote(
            part_sib.at[head], part_in.at[head], sent.at[5], c_recv.at[b], chip, 1 - core
        )

    def share(group):
        heads = [chip_at(b, 1) for b in group]
        turned = jnp.concatenate([att[:, cols(head)].T for head in heads], axis=0)
        theirs = jnp.dot(turned, g_sib[...], preferred_element_type=jnp.float32).astype(jnp.bfloat16)
        for i, head in enumerate(heads):
            part_sib[head] = theirs[i * HEAD : (i + 1) * HEAD]
        for b in group:
            core_copy(b).start()
        ours = jnp.dot(turned, g_own[...], preferred_element_type=jnp.float32)
        for i, head in enumerate(heads):
            part_own[head] = ours[i * HEAD : (i + 1) * HEAD]

    def z_copy(head, d):
        return pltpu.make_async_remote_copy(
            src_ref=tiles[0][0].at[head // 4, head % 4], dst_ref=landed[0][0].at[d - 1, head // 4],
            send_sem=r_send.at[0, 0], recv_sem=r_recv.at[0, 0], device_id=peer("z", d), device_id_type=MESH,
        )

    def y_copy(head, d):
        return pltpu.make_async_remote_copy(
            src_ref=tiles[1][0].at[head, (row_y + d) % 4], dst_ref=landed[1][0].at[d - 1, head],
            send_sem=r_send.at[1, 0], recv_sem=r_recv.at[1, 0], device_id=peer("y", d), device_id_type=MESH,
        )

    def x_copy(hi, part, d):
        to = (x + d) % 4
        at = pl.ds(hi * 4, 4)
        return pltpu.make_async_remote_copy(
            src_ref=tiles[2][0].at[part, at, to // 2], dst_ref=landed[2][0].at[d - 1, at],
            send_sem=r_send.at[2, 0], recv_sem=r_recv.at[2, 0], device_id=peer("x", d), device_id_type=MESH,
        )

    def join_cores(b):
        core_copy(b).wait_recv()
        head = chip_at(b, 1)
        both = part_own[head] + part_in[head].astype(jnp.float32)
        a0, a1 = PARTS[0], PARTS[0] + PARTS[1]
        lo, hi = head // 4, head % 4
        tiles[0][0][lo, hi] = both[:, 0:a0].astype(jnp.bfloat16).reshape(8, 16, a0)
        tiles[1][0][head] = both[:, a0:a1].astype(jnp.bfloat16).reshape(4, 2, 16, a1 - a0)
        tiles[2][0][lo, pl.ds(hi * 4, 4)] = (
            both[:, a1:].astype(jnp.bfloat16).reshape(4, 2, 16, half - a1)
        )
        dz = (hi - z + 4) % 4

        @pl.when(dz > 0)
        def _():
            z_copy(head, dz).start()

        for d in (1, 3, 2):
            y_copy(head, d).start()
        for to_hi in range(2):
            dx = (to_hi * 2 + lo - x + 4) % 4

            @pl.when(dx > 0)
            def _():
                x_copy(hi, lo, dx).start()

    for i, group in enumerate(HOME):
        for b in group:
            if b:
                out_copy(b).wait_recv()
        share(group)
        if i:
            for b in HOME[i - 1]:
                join_cores(b)
    for b in HOME[-1]:
        join_cores(b)

    def block(part, stage, d):
        tile = tiles[part][stage]
        axis = ORDERS[part][stage]
        if axis == "x":
            to = (x + d) % 4
            if part == 0:
                return tile.at[to % 2, to // 2]
            return tile.at[to % 2, :, to // 2]
        to = ((z if axis == "z" else row_y) + d) % 4
        if (part, stage) in ((0, 0), (0, 1), (1, 0)):
            return tile.at[:, to]
        return tile.at[to]

    def block_copy(part, stage, d):
        return pltpu.make_async_remote_copy(
            src_ref=block(part, stage, d), dst_ref=landed[part][stage].at[d - 1],
            send_sem=r_send.at[part, stage], recv_sem=r_recv.at[part, stage],
            device_id=peer(ORDERS[part][stage], d), device_id_type=MESH,
        )

    def send(part, stage):
        for d in (1, 3, 2):
            block_copy(part, stage, d).start()

    def total(part, stage):
        settle(landed[part][stage], r_recv.at[part, stage])
        value = block(part, stage, 0)[...].astype(jnp.float32)
        for d in range(3):
            value = value + landed[part][stage][d].astype(jnp.float32)
        return value

    def mix(i, unused):
        at = pl.ds(pl.multiple_of(i * 512, 512), 512)
        mixed[:, at] = jnp.dot(att[...], w_buf[:, at], preferred_element_type=jnp.float32).astype(
            jnp.bfloat16
        )
        return unused

    lax.fori_loop(0, w_buf.shape[1] // 512, mix, 0)
    mixed_copy = pltpu.make_async_copy(mixed, mixed_ref, local_sem.at[7])
    mixed_copy.start()

    for part in FIRST:
        tiles[part][1][...] = total(part, 0).astype(jnp.bfloat16).reshape(tiles[part][1].shape)
        send(part, 1)

    def last_copies(part):
        copies = []
        for d in (0, 1, 3, 2):
            for other in range(2):
                if d or other:
                    slot = 3 + d if other else d - 1
                    to = (core + other) % 2
                    target = dict(peer(ORDERS[part][2], d))
                    target["seq"] = target.get("seq", seq) + to - core
                    copies.append(
                        pltpu.make_async_remote_copy(
                            src_ref=block(part, 2, d).at[to], dst_ref=landed[part][2].at[slot],
                            send_sem=r_send.at[part, 2], recv_sem=r_recv.at[part, 2],
                            device_id=target, device_id_type=MESH,
                        )
                    )
        return copies

    for part in FIRST:
        tiles[part][2][...] = total(part, 1).reshape(tiles[part][2].shape)
        for copy in last_copies(part):
            copy.start()
    for part in FIRST:
        at = sum(PARTS[:part])
        settle(landed[part][2], r_recv.at[part, 2])
        ours = block(part, 2, 0).at[core][...]
        for d in range(3):
            ours = ours + landed[part][2][d]
        theirs = landed[part][2][3]
        for d in range(4, 7):
            theirs = theirs + landed[part][2][d]
        grad[:, pl.ds(pl.multiple_of(core * half + at, HEAD), PARTS[part])] = ours
        grad[:, pl.ds(pl.multiple_of((1 - core) * half + at, HEAD), PARTS[part])] = theirs

    mixed_copy.wait()
    some = (CHIPS - 1) * rows
    settle(ends.at[0 : 2 * CHIPS - 1], sent.at[0])
    settle(qq.at[0:some, 0:HEAD], sent.at[1])
    settle(kk.at[0 : 2 * some, 0:HEAD], sent.at[2])
    settle(kk.at[:, 0:HEAD], sent.at[3])
    settle(obuf.at[0:some, :], sent.at[4])
    settle(part_sib, sent.at[5])
    for part in range(3):
        for stage in range(3):
            settle(landed[part][stage], r_send.at[part, stage])


def attend(q, k, v, ends, w, g):
    rows, width = q.shape
    out = w.shape[1]
    half = out // 2
    pair = 2 * rows
    tokens = CHIPS * pair
    mine = CHIPS * rows
    dma = pltpu.SemaphoreType.DMA
    bf16 = jnp.bfloat16
    p0, p1, p2 = PARTS
    tiles = (
        (
            pltpu.VMEM((2, 4, 8, 16, p0), bf16),
            pltpu.VMEM((2, 4, 2, 16, p0), bf16),
            pltpu.VMEM((2, 2, 2, 8, p0), jnp.float32),
        ),
        (
            pltpu.VMEM((8, 4, 2, 16, p1), bf16),
            pltpu.VMEM((2, 4, 2, 16, p1), bf16),
            pltpu.VMEM((4, 2, 8, p1), jnp.float32),
        ),
        (
            pltpu.VMEM((2, 16, 2, 16, p2), bf16),
            pltpu.VMEM((4, 4, 16, p2), bf16),
            pltpu.VMEM((4, 2, 8, p2), jnp.float32),
        ),
    )
    landed = (
        (
            pltpu.VMEM((3, 2, 8, 16, p0), bf16),
            pltpu.VMEM((3, 2, 2, 16, p0), bf16),
            pltpu.VMEM((7, 8, p0), jnp.float32),
        ),
        (
            pltpu.VMEM((3, 8, 2, 16, p1), bf16),
            pltpu.VMEM((3, 4, 16, p1), bf16),
            pltpu.VMEM((7, 8, p1), jnp.float32),
        ),
        (
            pltpu.VMEM((3, 16, 16, p2), bf16),
            pltpu.VMEM((3, 4, 16, p2), bf16),
            pltpu.VMEM((7, 8, p2), jnp.float32),
        ),
    )
    return pl.pallas_call(
        functools.partial(attend_kernel, rows),
        out_shape=(
            jax.ShapeDtypeStruct((rows, out), bf16),
            jax.ShapeDtypeStruct((8, out), jnp.float32),
        ),
        in_specs=[pl.BlockSpec(memory_space=pl.ANY)] * 6,
        out_specs=(pl.BlockSpec(memory_space=pl.ANY), pl.BlockSpec(memory_space=pltpu.VMEM)),
        scratch_shapes=[
            pltpu.VMEM((mine, 2 * HEAD), bf16),
            pltpu.VMEM((tokens, 2 * HEAD), bf16),
            pltpu.VMEM((tokens, HEAD), bf16),
            pltpu.VMEM((HEAD + ONES, tokens), bf16),
            pltpu.VMEM((2 * CHIPS, 1, rows), jnp.int32),
            pltpu.VMEM((HEAD + ONES, mine), jnp.float32),
            pltpu.VMEM((8, mine), jnp.float32),
            pltpu.VMEM((GROUP, 2 * pair, WIDE), jnp.float32),
            pltpu.VMEM((GROUP, 8, WIDE), jnp.float32),
            pltpu.VMEM((mine, HEAD), bf16),
            dma((8,)),
            dma((4,)), dma((CHIPS,)), dma((4,)), dma((CHIPS,)), dma((CHIPS,)), dma((1,)),
            dma((3, 3)), dma((3, 3)), dma((6,)),
            pltpu.VMEM((rows, width), bf16),
            pltpu.VMEM((width, out), bf16),
            pltpu.VMEM((rows, half), bf16),
            pltpu.VMEM((rows, half), bf16),
            pltpu.VMEM((rows, out), bf16),
            pltpu.VMEM((CHIPS, HEAD, half), jnp.float32),
            pltpu.VMEM((CHIPS, HEAD, half), bf16),
            pltpu.VMEM((CHIPS, HEAD, half), bf16),
            tiles,
            landed,
        ],
        compiler_params=pltpu.CompilerParams(
            collective_id=0, has_side_effects=True, vmem_limit_bytes=60 << 20
        ),
    )(q, k, v, ends, w, g)


def hand_over_kernel(mixed_ref, grad_ref, mixed_out_ref, grad_out_ref, mixed, grad, sem):
    rows = mixed.shape[0] // PIECES
    arrays = [(grad_ref, grad_out_ref, grad)]
    for i in range(PIECES):
        at = pl.ds(i * rows, rows)
        arrays.append((mixed_ref.at[at, :], mixed_out_ref.at[at, :], mixed.at[at, :]))
    into = [
        pltpu.make_async_copy(source, held, sem.at[0, i]) for i, (source, _, held) in enumerate(arrays)
    ]
    out = [
        pltpu.make_async_copy(held, target, sem.at[1, i]) for i, (_, target, held) in enumerate(arrays)
    ]
    for copy in into:
        copy.start()
    for i in range(len(arrays)):
        into[i].wait()
        out[i].start()
    for copy in out:
        copy.wait()


def hand_over(mixed, grad):
    any_space = pl.BlockSpec(memory_space=pl.ANY)
    return pl.pallas_call(
        hand_over_kernel,
        out_shape=(
            jax.ShapeDtypeStruct(mixed.shape, mixed.dtype),
            jax.ShapeDtypeStruct(grad.shape, grad.dtype),
        ),
        in_specs=[any_space] * 2,
        out_specs=(any_space,) * 2,
        scratch_shapes=[
            pltpu.VMEM(mixed.shape, mixed.dtype),
            pltpu.VMEM(grad.shape, grad.dtype),
            pltpu.SemaphoreType.DMA((2, PIECES + 1)),
        ],
        compiler_params=pltpu.CompilerParams(vmem_limit_bytes=60 << 20),
    )(mixed, grad)


def body(query_rows, key_rows, value_rows, scale_end, out_weight, grad_out):
    mixed_out, out_grad = hand_over(
        *attend(query_rows[0], key_rows[0], value_rows[0], scale_end, out_weight, grad_out[0])
    )
    return (mixed_out[None], out_grad)


def solution(mesh):
    torus = Mesh(mesh.devices.reshape(2, 4, mesh.shape["seq"]), ("dp_0", "dp_1", "seq"))
    in_specs = (
        P(DP, "seq", None),
        P(DP, "seq", None),
        P(DP, "seq", None),
        P("seq"),
        P(),
        P(DP, "seq", None),
    )
    out_specs = (P(DP, "seq", None), P(DP_SEQ, None))
    return jax.shard_map(body, mesh=torus, in_specs=in_specs, out_specs=out_specs, check_vma=False)
```
